16 devices in a mesh: data: 16 (over z, y, x, core).
Axes of the slice: x: 2, y: 2, z: 2, core: 2. Of those that a mesh axis runs over, the one named last changes fastest.
Arguments:
- x_in: bfloat16 [48, 512, 2048], P('data')
- dy_out: bfloat16 [48, 512, 2048], P('data')
- lengths: int32 [48], P('data')
- w_up: bfloat16 [2, 2048, 8192], replicated
- w_down: bfloat16 [2, 8192, 2048], replicated
- noise_up: float32 [2, 2048, 8192], replicated
- noise_down: float32 [2, 8192, 2048], replicated
- clip_norm: float32 [2], replicated
Outputs:
- output 1: float32 [2, 2048, 8192], replicated
- output 2: float32 [2, 8192, 2048], replicated
All inputs are finite; a program needn't handle non-finite values.
Results may differ from the reference program's by a relative error of at most 0.0112315.
Values are sent between devices in bfloat16 or wider.
A program may use at most 2.75 GiB of HBM per device.

```python
import jax
import jax.numpy as jnp
from jax import lax

D = 2048
SEQ = 512
SAMP_DEV = 3
DATA = 16
LAYERS = 2
FF = 4 * D
BATCH = SAMP_DEV * DATA


def setup_inputs(seed: int = 0) -> dict:
    key_list = jax.random.split(jax.random.key(seed), 9)
    lengths = jax.random.randint(key_list[0], (BATCH,), SEQ // 4, SEQ + 1)
    lengths = lengths.at[0].set(SEQ).at[1].set(SEQ // 4)
    big_flag = jax.random.randint(key_list[1], (BATCH,), 0, 2)
    row_scale = jnp.where(big_flag == 1, 1.8, 0.45) * jnp.sqrt(SEQ / lengths.astype(jnp.float32))
    x_in = jax.random.normal(key_list[2], (BATCH, SEQ, D), jnp.float32)
    dy_out = jax.random.normal(key_list[3], (BATCH, SEQ, D), jnp.float32) * row_scale[:, None, None]
    w_up = jax.random.normal(key_list[4], (LAYERS, D, FF), jnp.float32) * D ** -0.5
    w_down = jax.random.normal(key_list[5], (LAYERS, FF, D), jnp.float32) * (FF * LAYERS) ** -0.5
    share_up = 0.12 / LAYERS
    share_down = 0.45
    base_norm = (SEQ * FF * D * (1.0 + 0.45 / LAYERS) ** (LAYERS - 1) * (share_up + share_down)) ** 0.5
    clip_norm = base_norm * jax.random.uniform(key_list[6], (LAYERS,), jnp.float32, 0.8, 1.2)
    noise_unit = 0.4 * BATCH ** 0.5 * clip_norm / (D * FF) ** 0.5
    up_std = noise_unit * (share_up / (share_up + share_down)) ** 0.5
    down_std = noise_unit * (share_down / (share_up + share_down)) ** 0.5
    noise_up = jax.random.normal(key_list[7], (LAYERS, D, FF), jnp.float32) * up_std[:, None, None]
    noise_down = jax.random.normal(key_list[8], (LAYERS, FF, D), jnp.float32) * down_std[:, None, None]
    return {'x_in': x_in.astype(jnp.bfloat16), 'dy_out': dy_out.astype(jnp.bfloat16), 'lengths': lengths.astype(jnp.int32), 'w_up': w_up.astype(jnp.bfloat16), 'w_down': w_down.astype(jnp.bfloat16), 'noise_up': noise_up, 'noise_down': noise_down, 'clip_norm': clip_norm}


def gelu_grad(hidden):
    return 0.5 * (1.0 + lax.erf(hidden * 0.7071067811865476)) + hidden * jnp.exp(-0.5 * hidden * hidden) * 0.3989422804014327


def gram_of(matrix):
    blocks = matrix.reshape(SAMP_DEV, SEQ, matrix.shape[-1]).astype(jnp.float32)
    return jnp.einsum('btk,bsk->bts', blocks, blocks)


def block_sums(x_block, dy_block, len_block, w_up, w_down, clip_norm):
    n_rows = SAMP_DEV * SEQ
    tok_mask = jnp.arange(SEQ)[None, :] < len_block[:, None]
    grad_cur = jnp.where(tok_mask[:, :, None], dy_block, jnp.zeros_like(dy_block)).reshape(n_rows, D)
    x_cur = x_block.reshape(n_rows, D)
    saved = []
    for layer_idx in range(LAYERS):
        hidden = jnp.dot(x_cur, w_up[layer_idx], preferred_element_type=jnp.float32).astype(jnp.bfloat16)
        gelu_out = jax.nn.gelu(hidden.astype(jnp.float32), approximate=False).astype(jnp.bfloat16)
        saved.append((x_cur, hidden, gelu_out))
        if layer_idx < LAYERS - 1:
            x_cur = (x_cur.astype(jnp.float32) + jnp.dot(gelu_out, w_down[layer_idx], preferred_element_type=jnp.float32)).astype(jnp.bfloat16)
    up_sums = []
    down_sums = []
    for layer_idx in reversed(range(LAYERS)):
        x_cur, hidden, gelu_out = saved[layer_idx]
        grad_act = jnp.dot(grad_cur, w_down[layer_idx].T, preferred_element_type=jnp.float32)
        grad_pre = (grad_act * gelu_grad(hidden.astype(jnp.float32))).astype(jnp.bfloat16)
        norm_sq = jnp.sum(gram_of(gelu_out) * gram_of(grad_cur) + gram_of(x_cur) * gram_of(grad_pre), axis=(1, 2))
        factor = jnp.minimum(1.0, clip_norm[layer_idx] / jnp.sqrt(norm_sq))
        row_factor = jnp.broadcast_to(factor[:, None], (SAMP_DEV, SEQ)).reshape(n_rows, 1)
        grad_clip = (grad_cur.astype(jnp.float32) * row_factor).astype(jnp.bfloat16)
        pre_clip = (grad_pre.astype(jnp.float32) * row_factor).astype(jnp.bfloat16)
        up_sums.append(jnp.dot(x_cur.T, pre_clip, preferred_element_type=jnp.float32))
        down_sums.append(jnp.dot(gelu_out.T, grad_clip, preferred_element_type=jnp.float32))
        if layer_idx > 0:
            grad_cur = (grad_cur.astype(jnp.float32) + jnp.dot(grad_pre, w_up[layer_idx].T, preferred_element_type=jnp.float32)).astype(jnp.bfloat16)
    return jnp.stack(up_sums[::-1]), jnp.stack(down_sums[::-1])


def reference(x_in, dy_out, lengths, w_up, w_down, noise_up, noise_down, clip_norm):
    def scan_step(run_sums, block):
        up_part, down_part = block_sums(block[0], block[1], block[2], w_up, w_down, clip_norm)
        return (run_sums[0] + up_part, run_sums[1] + down_part), None
    init_sums = (jnp.zeros((LAYERS, D, FF), jnp.float32), jnp.zeros((LAYERS, FF, D), jnp.float32))
    blocks = (x_in.reshape(DATA, SAMP_DEV, SEQ, D), dy_out.reshape(DATA, SAMP_DEV, SEQ, D), lengths.reshape(DATA, SAMP_DEV))
    total_sums, _ = lax.scan(scan_step, init_sums, blocks)
    return (total_sums[0] + noise_up) / BATCH, (total_sums[1] + noise_down) / BATCH
```

```python
import functools
import jax
import jax.numpy as jnp
from jax import lax
from jax.experimental import pallas as pl
from jax.experimental.pallas import tpu as pltpu
from jax.sharding import PartitionSpec as P

F32 = jnp.float32
BF16 = jnp.bfloat16
MESH_ID = pl.DeviceIdType.MESH
ANY = pl.BlockSpec(memory_space=pl.ANY)
CW = 256
PER_MAT = 16
CHUNKS = 2 * PER_MAT
LAG1, LAG2, LAG3 = 4, 7, 10
RECV = 6
OWN = 10


def normal_cdf(z):
    return 0.5 * (1.0 + lax.erf(z * 0.7071067811865476))


def dot_nt(a, b):
    return lax.dot_general(a, b, (((1,), (1,)), ((), ())), preferred_element_type=F32)


def up_kernel(x_ref, w_ref, z_ref, a_ref):
    for start in range(0, x_ref.shape[0], 512):
        rows = pl.ds(start, 512)
        z = jnp.dot(x_ref[rows, :], w_ref[0], preferred_element_type=F32).astype(BF16)
        z_ref[rows, :] = z
        zf = z.astype(F32)
        a_ref[rows, :] = (zf * normal_cdf(zf)).astype(BF16)


def forward_up(layer, x_rows, w_up):
    n_rows, dim = x_rows.shape
    ff = w_up.shape[2]
    tile = 512
    out = jax.ShapeDtypeStruct((n_rows, ff), BF16)
    col = pl.BlockSpec((n_rows, tile), lambda j: (0, j))
    return pl.pallas_call(
        up_kernel, out_shape=(out, out), grid=(ff // tile,),
        in_specs=[pl.BlockSpec((n_rows, dim), lambda j: (0, 0)), pl.BlockSpec((1, dim, tile), lambda j: (layer, 0, j))],
        out_specs=(col, col), name='forward_up',
        cost_estimate=pl.CostEstimate(flops=2 * n_rows * dim * ff, bytes_accessed=dim * ff * 2 + n_rows * ff * 4, transcendentals=n_rows * ff),
        compiler_params=pltpu.CompilerParams(vmem_limit_bytes=56 * 1024 * 1024))(x_rows, w_up)


def add_kernel(transposed, a_ref, w_ref, x_ref, o_ref, acc):
    k = pl.program_id(1)

    @pl.when(k == 0)
    def _():
        acc[...] = x_ref[...].astype(F32)

    for start in range(0, a_ref.shape[0], 512):
        rows = pl.ds(start, 512)
        if transposed:
            acc[rows, :] += dot_nt(a_ref[rows, :], w_ref[0])
        else:
            acc[rows, :] += jnp.dot(a_ref[rows, :], w_ref[0], preferred_element_type=F32)

    @pl.when(k == pl.num_programs(1) - 1)
    def _():
        o_ref[...] = acc[...].astype(BF16)


def add_product(layer, x_rows, a_rows, weight, transposed):
    n_rows, dim = x_rows.shape
    ff = a_rows.shape[1]
    tn, tk = 1024, 2048
    if transposed:
        w_spec = pl.BlockSpec((1, tn, tk), lambda n, k: (layer, n, k))
    else:
        w_spec = pl.BlockSpec((1, tk, tn), lambda n, k: (layer, k, n))
    col = pl.BlockSpec((n_rows, tn), lambda n, k: (0, n))
    return pl.pallas_call(
        functools.partial(add_kernel, transposed), out_shape=jax.ShapeDtypeStruct((n_rows, dim), BF16), grid=(dim // tn, ff // tk),
        in_specs=[pl.BlockSpec((n_rows, tk), lambda n, k: (0, k)), w_spec, col],
        out_specs=col, scratch_shapes=[pltpu.VMEM((n_rows, tn), F32)], name='add_product',
        cost_estimate=pl.CostEstimate(flops=2 * n_rows * dim * ff, bytes_accessed=dim * ff * 2 + n_rows * ff * 4, transcendentals=0),
        compiler_params=pltpu.CompilerParams(vmem_limit_bytes=60 * 1024 * 1024))(a_rows, weight, x_rows)


def grad_kernel(has_hidden, n_samples, clip_ref, x_ref, g_ref, *refs):
    if has_hidden:
        z_ref, a_ref, wd_ref, h_ref, f_ref, gram_a, gram_h = refs
    else:
        wu_ref, wd_ref, a_ref, h_ref, f_ref, gram_a, gram_h = refs
    j = pl.program_id(0)
    seq = x_ref.shape[0] // n_samples
    half = seq // 2
    low, high = slice(0, half), slice(half, seq)

    @pl.when(j == 0)
    def _():
        gram_a[...] = jnp.zeros_like(gram_a)
        gram_h[...] = jnp.zeros_like(gram_h)

    for s in range(n_samples):
        rows = pl.ds(s * seq, seq)
        if has_hidden:
            z = z_ref[rows, :].astype(F32)
        else:
            z = jnp.dot(x_ref[rows, :], wu_ref[0], preferred_element_type=F32).astype(BF16).astype(F32)
        u = dot_nt(g_ref[rows, :], wd_ref[0])
        cdf = normal_cdf(z)
        if has_hidden:
            a = a_ref[rows, :]
        else:
            a = (z * cdf).astype(BF16)
            a_ref[rows, :] = a
        h = (u * (cdf + z * jnp.exp(-0.5 * z * z) * 0.3989422804014327)).astype(BF16)
        h_ref[rows, :] = h
        gram_a[s, low, low] += dot_nt(a[low], a[low])
        gram_a[s, high, :] += dot_nt(a[high], a)
        gram_h[s, low, low] += dot_nt(h[low], h[low])
        gram_h[s, high, :] += dot_nt(h[high], h)

    @pl.when(j == pl.num_programs(0) - 1)
    def _():
        for s in range(n_samples):
            first, second = pl.ds(s * seq, half), pl.ds(s * seq + half, half)

            def paired(r, rr, c, cc):
                gg = dot_nt(g_ref[rr, :], g_ref[cc, :])
                xx = dot_nt(x_ref[rr, :], x_ref[cc, :])
                return gram_a[s, r, c] * gg + gram_h[s, r, c] * xx

            total = paired(low, first, low, first) + paired(high, second, high, second) + 2.0 * paired(high, second, low, first)
            norm_sq = jnp.sum(total, axis=(0, 1), keepdims=True)
            factor = jnp.minimum(1.0, clip_ref[0] / jnp.sqrt(norm_sq))
            f_ref[pl.ds(s * seq, seq), :] = jnp.broadcast_to(factor, (seq, 1))


def block_grad(layer, x_rows, g_rows, hidden, w_up, w_down, clip, n_samples):
    n_rows, dim = x_rows.shape
    ff = w_up.shape[2]
    tile = 512
    seq = n_rows // n_samples
    col = pl.BlockSpec((n_rows, tile), lambda j: (0, j))
    whole = pl.BlockSpec((n_rows, dim), lambda j: (0, 0), pipeline_mode=pl.Buffered(buffer_count=1))
    wd_spec = pl.BlockSpec((1, tile, dim), lambda j: (layer, j, 0))
    rows_spec = pl.BlockSpec((n_rows, 1), lambda j: (0, 0))
    big = jax.ShapeDtypeStruct((n_rows, ff), BF16)
    row_out = jax.ShapeDtypeStruct((n_rows, 1), F32)
    smem = pl.BlockSpec(memory_space=pltpu.SMEM)
    products = 2 if hidden is None else 1
    if hidden is None:
        in_specs = [smem, whole, whole, pl.BlockSpec((1, dim, tile), lambda j: (layer, 0, j)), wd_spec]
        args = (clip, x_rows, g_rows, w_up, w_down)
        out_shape, out_specs = (big, big, row_out), (col, col, rows_spec)
    else:
        in_specs = [smem, whole, whole, col, col, wd_spec]
        args = (clip, x_rows, g_rows, hidden[0], hidden[1], w_down)
        out_shape, out_specs = (big, row_out), (col, rows_spec)
    return pl.pallas_call(
        functools.partial(grad_kernel, hidden is not None, n_samples), out_shape=out_shape, grid=(ff // tile,), in_specs=in_specs, out_specs=out_specs,
        scratch_shapes=[pltpu.VMEM((n_samples, seq, seq), F32)] * 2, name='block_grad',
        cost_estimate=pl.CostEstimate(flops=(2 * products * dim + 3 * seq) * n_rows * ff, bytes_accessed=dim * ff * 4 + n_rows * ff * 4, transcendentals=2 * n_rows * ff),
        compiler_params=pltpu.CompilerParams(vmem_limit_bytes=60 * 1024 * 1024))(*args)


def axis_weight(axis):
    return 2 * (axis + 1) + 2 * (axis // 2)


def sums_kernel(shift, x_hbm, h_hbm, a_hbm, g_hbm, rowf, r_hbm, lt, slab, gpiece, clip, own, s0s, s0r, rc1, rc2, rc3, obuf,
                slab_sem, g_sem, o_sem, d_send, d_recv, sems_s, sems_r):
    me = lax.axis_index('data')
    core = me % 2
    partner = me + 1 - 2 * core

    def bit_peer(chunk, stage):
        axis = (chunk + shift + stage) % 3
        weight = axis_weight(axis)
        bit = (me // weight) % 2
        return bit, me + weight * (1 - 2 * bit)

    barrier = pltpu.get_barrier_semaphore()
    pl.semaphore_signal(barrier, inc=1, device_id=(partner,), device_id_type=MESH_ID)
    for axis in range(3):
        weight = axis_weight(axis)
        peer = me + weight * (1 - 2 * ((me // weight) % 2))
        pl.semaphore_signal(barrier, inc=1, device_id=(peer,), device_id_type=MESH_ID)
    pl.semaphore_wait(barrier, 4)

    def columns(half, chunk):
        return pl.ds(pl.multiple_of((half * PER_MAT + chunk % PER_MAT) * CW, CW), CW)

    def start_slab(half, chunk, buf):
        @pl.when(chunk < PER_MAT)
        def _():
            pltpu.make_async_copy(h_hbm.at[:, columns(half, chunk)], slab.at[buf], slab_sem.at[buf]).start()

        @pl.when(chunk >= PER_MAT)
        def _():
            pltpu.make_async_copy(a_hbm.at[:, columns(half, chunk)], slab.at[buf], slab_sem.at[buf]).start()

    def wait_slab(buf):
        pltpu.make_async_copy(h_hbm.at[:, pl.ds(0, CW)], slab.at[buf], slab_sem.at[buf]).wait()

    def x_copy(piece):
        return pltpu.make_async_copy(x_hbm.at[:, pl.ds(piece * CW, CW)], slab.at[piece % 4], slab_sem.at[piece % 4])

    n_pieces = x_hbm.shape[1] // CW
    for piece in range(3):
        x_copy(piece).start()
    for piece in range(n_pieces):
        if piece + 3 < n_pieces:
            x_copy(piece + 3).start()
        x_copy(piece).wait()
        lt[0, pl.ds(piece * CW, CW), :] = slab[piece % 4].T

    def g_copy(piece):
        return pltpu.make_async_copy(g_hbm.at[:, pl.ds(pl.multiple_of(piece * CW, CW), CW)], gpiece, g_sem)

    def load_clip(chunk, buf):
        scale = jnp.where(chunk < PER_MAT, rowf[...], 1.0)
        clip[...] = (slab[buf].astype(F32) * scale).astype(BF16)

    def partner_chunk(chunk):
        buf = chunk % 2
        wait_slab(buf)
        load_clip(chunk, buf)

        @pl.when(chunk + 1 < CHUNKS)
        def _():
            start_slab(1 - core, chunk + 1, 1 - buf)

        mat = chunk // PER_MAT
        for q in range(4):
            rows = pl.ds(q * 512, 512)
            s0s[buf, rows, :] = jnp.dot(lt[mat, rows, :], clip[...], preferred_element_type=F32).astype(BF16)

    def d2d(chunk):
        buf = chunk % 2
        return pltpu.make_async_remote_copy(s0s.at[buf], s0r.at[buf], d_send.at[buf], d_recv.at[buf], device_id=(partner,), device_id_type=MESH_ID)

    def own_chunk(chunk):
        buf = 2 + chunk % 2
        wait_slab(buf)
        load_clip(chunk, buf)

        @pl.when(chunk + 1 < CHUNKS)
        def _():
            start_slab(core, chunk + 1, 5 - buf)

        d2d(chunk).wait()
        mat = chunk // PER_MAT
        for q in range(4):
            rows = pl.ds(q * 512, 512)
            part = jnp.dot(lt[mat, rows, :], clip[...], preferred_element_type=F32)
            own[chunk % OWN, rows, :] = (part + s0r[chunk % 2, rows, :].astype(F32)).astype(BF16)

    def kept_row(chunk, stage):
        row = 0
        for s in range(stage):
            bit, _ = bit_peer(chunk, s)
            row = row + bit * (1024 // (2 ** s))
        return row

    recv_bufs = (rc1, rc2, rc3)

    def stage_copy(chunk, stage):
        size = 1024 // (2 ** stage)
        bit, peer = bit_peer(chunk, stage)
        row = kept_row(chunk, stage) + (1 - bit) * size
        slot = chunk % RECV
        return pltpu.make_async_remote_copy(
            own.at[chunk % OWN, pl.ds(pl.multiple_of(row, CW), size), :], recv_bufs[stage].at[slot],
            sems_s.at[stage, slot], sems_r.at[stage, slot], device_id=(peer,), device_id_type=MESH_ID)

    def stage_sum(chunk, stage):
        size = 1024 // (2 ** stage)
        rows = pl.ds(pl.multiple_of(kept_row(chunk, stage + 1), CW), size)
        return rows, own[chunk % OWN, rows, :].astype(F32) + recv_bufs[stage][chunk % RECV].astype(F32)

    def out_copy(chunk):
        return pltpu.make_async_copy(obuf.at[chunk % 2], r_hbm.at[chunk], o_sem.at[chunk % 2])

    start_slab(1 - core, 0, 0)
    start_slab(core, 0, 2)
    partner_chunk(0)
    g_copy(0).start()
    d2d(0).start()

    def step(t, _):
        @pl.when(t >= LAG3)
        def _():
            chunk = t - LAG3
            stage_copy(chunk, 2).wait()
            _, total = stage_sum(chunk, 2)

            @pl.when(chunk >= 2)
            def _():
                out_copy(chunk - 2).wait()

            @pl.when(chunk < PER_MAT)
            def _():
                obuf[chunk % 2] = total.astype(BF16)

            @pl.when(chunk >= PER_MAT)
            def _():
                obuf[chunk % 2] = total.T.astype(BF16)

            out_copy(chunk).start()

        @pl.when((t >= LAG2) & (t < CHUNKS + LAG2))
        def _():
            chunk = t - LAG2
            stage_copy(chunk, 1).wait()
            rows, total = stage_sum(chunk, 1)
            own[chunk % OWN, rows, :] = total.astype(BF16)

        @pl.when((t >= LAG1) & (t < CHUNKS + LAG1))
        def _():
            chunk = t - LAG1
            stage_copy(chunk, 0).wait()
            rows, total = stage_sum(chunk, 0)
            own[chunk % OWN, rows, :] = total.astype(BF16)

        @pl.when((t >= 1) & (t < CHUNKS + 1))
        def _():
            stage_copy(t - 1, 0).start()

        @pl.when(t < n_pieces)
        def _():
            g_copy(t).wait()
            lt[1, pl.ds(pl.multiple_of(t * CW, CW), CW), :] = (gpiece[...].astype(F32) * rowf[...]).astype(BF16).T

            @pl.when(t + 1 < n_pieces)
            def _():
                g_copy(t + 1).start()

        @pl.when(t < CHUNKS - 1)
        def _():
            partner_chunk(t + 1)

        @pl.when(t < CHUNKS)
        def _():
            own_chunk(t)

        @pl.when(t < CHUNKS - 1)
        def _():
            d2d(t + 1).start()

        @pl.when((t >= LAG1) & (t < CHUNKS + LAG1))
        def _():
            stage_copy(t - LAG1, 1).start()

        @pl.when((t >= LAG2) & (t < CHUNKS + LAG2))
        def _():
            stage_copy(t - LAG2, 2).start()

        return 0

    lax.fori_loop(0, CHUNKS + LAG3, step, 0)
    out_copy(CHUNKS - 2).wait()
    out_copy(CHUNKS - 1).wait()


def block_sums(layer, x_rows, h_rows, a_rows, g_rows, row_factor):
    n_rows, dim = x_rows.shape
    scratch = [
        pltpu.VMEM((2, dim, n_rows), BF16), pltpu.VMEM((4, n_rows, CW), BF16), pltpu.VMEM((n_rows, CW), BF16), pltpu.VMEM((n_rows, CW), BF16),
        pltpu.VMEM((OWN, dim, CW), BF16), pltpu.VMEM((2, dim, CW), BF16), pltpu.VMEM((2, dim, CW), BF16),
        pltpu.VMEM((RECV, dim // 2, CW), BF16), pltpu.VMEM((RECV, dim // 4, CW), BF16), pltpu.VMEM((RECV, dim // 8, CW), BF16),
        pltpu.VMEM((2, CW, CW), BF16),
        pltpu.SemaphoreType.DMA((4,)), pltpu.SemaphoreType.DMA, pltpu.SemaphoreType.DMA((2,)),
        pltpu.SemaphoreType.DMA((2,)), pltpu.SemaphoreType.DMA((2,)), pltpu.SemaphoreType.DMA((3, RECV)), pltpu.SemaphoreType.DMA((3, RECV)),
    ]
    flops = 4 * n_rows * dim * h_rows.shape[1]
    return pl.pallas_call(
        functools.partial(sums_kernel, 2 * layer),
        out_shape=jax.ShapeDtypeStruct((CHUNKS, CW, CW), BF16),
        in_specs=[ANY, ANY, ANY, ANY, pl.BlockSpec(memory_space=pltpu.VMEM)],
        out_specs=ANY,
        scratch_shapes=scratch,
        compiler_params=pltpu.CompilerParams(collective_id=layer, has_side_effects=True, vmem_limit_bytes=60 * 1024 * 1024),
        cost_estimate=pl.CostEstimate(flops=flops, bytes_accessed=4 * n_rows * h_rows.shape[1], transcendentals=0),
        name=f'sums_{layer}',
    )(x_rows, h_rows, a_rows, g_rows, row_factor)


def owner_of(chunk, piece, half, shift):
    color = (chunk + shift) % 3
    b1, b2, b3 = piece // 4, (piece // 2) % 2, piece % 2
    return b1 * axis_weight(color) + b2 * axis_weight((color + 1) % 3) + b3 * axis_weight((color + 2) % 3) + half


def finish_kernel(n_in, scale, *refs):
    pieces, noise, out = refs[:n_in], refs[n_in], refs[-1]
    for i in range(n_in):
        cols = pl.ds(i * CW, CW)
        out[0, :, cols] = (pieces[i][0, 0].astype(F32) + noise[0, :, cols]) * scale


def finish_up(layer, gathered, noise, prev, batch_total):
    layers, dim, ff = noise.shape
    shift = 2 * layer

    def piece_spec(c):
        return pl.BlockSpec((1, 1, CW, CW), lambda i, k, c=c: (owner_of(c, i, k, shift), c, 0, 0))

    tile = pl.BlockSpec((1, CW, ff // 2), lambda i, k: (layer, i, k))
    in_specs = [piece_spec(c) for c in range(PER_MAT)] + [tile]
    args = [gathered] * PER_MAT + [noise]
    aliases = {}
    if prev is not None:
        in_specs.append(ANY)
        args.append(prev)
        aliases = {len(args) - 1: 0}
    return pl.pallas_call(
        functools.partial(finish_kernel, PER_MAT, 1.0 / batch_total),
        out_shape=jax.ShapeDtypeStruct(noise.shape, F32), grid=(dim // CW, 2), in_specs=in_specs, out_specs=tile,
        input_output_aliases=aliases, name=f'finish_up_{layer}',
        cost_estimate=pl.CostEstimate(flops=dim * ff * 2, bytes_accessed=dim * ff * 10, transcendentals=0),
        compiler_params=pltpu.CompilerParams(vmem_limit_bytes=50 * 1024 * 1024))(*args)


def finish_down(layer, gathered, noise, prev, batch_total):
    layers, ff, dim = noise.shape
    shift = 2 * layer
    n_in = dim // CW

    def piece_spec(i):
        return pl.BlockSpec((1, 1, CW, CW), lambda k, c, i=i: (owner_of(c + PER_MAT, i, k, shift), c + PER_MAT, 0, 0))

    tile = pl.BlockSpec((1, CW, dim), lambda k, c: (layer, k * PER_MAT + c, 0))
    in_specs = [piece_spec(i) for i in range(n_in)] + [tile]
    args = [gathered] * n_in + [noise]
    aliases = {}
    if prev is not None:
        in_specs.append(ANY)
        args.append(prev)
        aliases = {len(args) - 1: 0}
    return pl.pallas_call(
        functools.partial(finish_kernel, n_in, 1.0 / batch_total),
        out_shape=jax.ShapeDtypeStruct(noise.shape, F32), grid=(2, PER_MAT), in_specs=in_specs, out_specs=tile,
        input_output_aliases=aliases, name=f'finish_down_{layer}',
        cost_estimate=pl.CostEstimate(flops=dim * ff * 2, bytes_accessed=dim * ff * 10, transcendentals=0),
        compiler_params=pltpu.CompilerParams(vmem_limit_bytes=50 * 1024 * 1024))(*args)


def per_device(x_in, dy_out, lengths, w_up, w_down, noise_up, noise_down, clip_norm, batch_total):
    n_samples, seq_len, dim = x_in.shape
    n_rows = n_samples * seq_len
    tok_mask = (jnp.arange(seq_len)[None, :] < lengths[:, None]).astype(BF16)
    g_last = (dy_out * tok_mask[:, :, None]).reshape(n_rows, dim)
    x_first = x_in.reshape(n_rows, dim)
    z_first, a_first = forward_up(0, x_first, w_up)
    x_last = add_product(0, x_first, a_first, w_down, False)
    a_last, h_last, row_factor = block_grad(1, x_last, g_last, None, w_up, w_down, clip_norm[1:], n_samples)
    piece = block_sums(1, x_last, h_last, a_last, g_last, row_factor)
    gathered = lax.all_gather(piece, 'data')
    g_first = add_product(1, g_last, h_last, w_up, True)
    h_first, row_factor = block_grad(0, x_first, g_first, (z_first, a_first), w_up, w_down, clip_norm[:1], n_samples)
    piece = block_sums(0, x_first, h_first, a_first, g_first, row_factor)
    gathered_first = lax.all_gather(piece, 'data')
    grad_up = finish_up(1, gathered, noise_up, None, batch_total)
    grad_down = finish_down(1, gathered, noise_down, None, batch_total)
    grad_up = finish_up(0, gathered_first, noise_up, grad_up, batch_total)
    grad_down = finish_down(0, gathered_first, noise_down, grad_down, batch_total)
    return grad_up, grad_down


def solution(mesh):
    batch_spec = P('data', None, None)

    def grad_step(x_in, dy_out, lengths, w_up, w_down, noise_up, noise_down, clip_norm):
        device_fn = functools.partial(per_device, batch_total=x_in.shape[0])
        mapped = jax.shard_map(device_fn, mesh=mesh, in_specs=(batch_spec, batch_spec, P('data'), P(), P(), P(), P(), P()), out_specs=(P(), P()), check_vma=False)
        return mapped(x_in, dy_out, lengths, w_up, w_down, noise_up, noise_down, clip_norm)

    return grad_step
```

```python
import functools
import jax
import jax.numpy as jnp
from jax import lax
from jax.experimental import pallas as pl
from jax.experimental.pallas import tpu as pltpu
from jax.sharding import PartitionSpec as P

F32 = jnp.float32
BF16 = jnp.bfloat16
MESH_ID = pl.DeviceIdType.MESH
ANY = pl.BlockSpec(memory_space=pl.ANY)
CW = 256
PER_MAT = 16
CHUNKS = 2 * PER_MAT
SPLIT = 24
LAG1, LAG2, LAG3 = 4, 7, 10
RECV = 6
OWN = 10


def normal_cdf(z):
    return 0.5 * (1.0 + lax.erf(z * 0.7071067811865476))


def dot_nt(a, b):
    return lax.dot_general(a, b, (((1,), (1,)), ((), ())), preferred_element_type=F32)


def forward_kernel(block, x_ref, wu_ref, wd_ref, z_ref, a_ref, o_ref, acc):
    j = pl.program_id(0)

    @pl.when(j == 0)
    def _():
        acc[...] = x_ref[...].astype(F32)

    for start in range(0, x_ref.shape[0], block):
        rows = pl.ds(start, block)
        z = jnp.dot(x_ref[rows, :], wu_ref[0], preferred_element_type=F32).astype(BF16)
        z_ref[rows, :] = z
        zf = z.astype(F32)
        a = (zf * normal_cdf(zf)).astype(BF16)
        a_ref[rows, :] = a
        acc[rows, :] += jnp.dot(a, wd_ref[0], preferred_element_type=F32)

    @pl.when(j == pl.num_programs(0) - 1)
    def _():
        o_ref[...] = acc[...].astype(BF16)


def resident(shape):
    return pl.BlockSpec(shape, lambda j: (0, 0), pipeline_mode=pl.Buffered(buffer_count=1))


def forward_block(layer, x_rows, w_up, w_down):
    n_rows, dim = x_rows.shape
    ff = w_up.shape[2]
    tile = 512
    big = jax.ShapeDtypeStruct((n_rows, ff), BF16)
    col = pl.BlockSpec((n_rows, tile), lambda j: (0, j))
    return pl.pallas_call(
        functools.partial(forward_kernel, n_rows // 2), out_shape=(big, big, jax.ShapeDtypeStruct((n_rows, dim), BF16)), grid=(ff // tile,),
        in_specs=[resident((n_rows, dim)), pl.BlockSpec((1, dim, tile), lambda j: (layer, 0, j)), pl.BlockSpec((1, tile, dim), lambda j: (layer, j, 0))],
        out_specs=(col, col, resident((n_rows, dim))), scratch_shapes=[pltpu.VMEM((n_rows, dim), F32)], name='forward_block',
        cost_estimate=pl.CostEstimate(flops=4 * n_rows * dim * ff, bytes_accessed=dim * ff * 4 + n_rows * ff * 4, transcendentals=n_rows * ff),
        compiler_params=pltpu.CompilerParams(vmem_limit_bytes=63 * 1024 * 1024))(x_rows, w_up, w_down)


def add_kernel(transposed, a_ref, w_ref, x_ref, o_ref, acc):
    k = pl.program_id(1)

    @pl.when(k == 0)
    def _():
        acc[...] = x_ref[...].astype(F32)

    for start in range(0, a_ref.shape[0], 512):
        rows = pl.ds(start, 512)
        if transposed:
            acc[rows, :] += dot_nt(a_ref[rows, :], w_ref[0])
        else:
            acc[rows, :] += jnp.dot(a_ref[rows, :], w_ref[0], preferred_element_type=F32)

    @pl.when(k == pl.num_programs(1) - 1)
    def _():
        o_ref[...] = acc[...].astype(BF16)


def add_product(layer, x_rows, a_rows, weight, transposed):
    n_rows, dim = x_rows.shape
    ff = a_rows.shape[1]
    tn, tk = 1024, 2048
    if transposed:
        w_spec = pl.BlockSpec((1, tn, tk), lambda n, k: (layer, n, k))
    else:
        w_spec = pl.BlockSpec((1, tk, tn), lambda n, k: (layer, k, n))
    col = pl.BlockSpec((n_rows, tn), lambda n, k: (0, n))
    return pl.pallas_call(
        functools.partial(add_kernel, transposed), out_shape=jax.ShapeDtypeStruct((n_rows, dim), BF16), grid=(dim // tn, ff // tk),
        in_specs=[pl.BlockSpec((n_rows, tk), lambda n, k: (0, k)), w_spec, col],
        out_specs=col, scratch_shapes=[pltpu.VMEM((n_rows, tn), F32)], name='add_product',
        cost_estimate=pl.CostEstimate(flops=2 * n_rows * dim * ff, bytes_accessed=dim * ff * 2 + n_rows * ff * 4, transcendentals=0),
        compiler_params=pltpu.CompilerParams(vmem_limit_bytes=60 * 1024 * 1024))(a_rows, weight, x_rows)


def grad_kernel(first, n_samples, clip_ref, len_ref, x_ref, g_in, *refs):
    if first:
        g_ref = g_in
        z_ref, a_ref, wd_ref, h_ref, fr_ref, f_ref, xt_ref, gt_ref, gram_a, gram_h = refs
    else:
        wu_ref, wd_ref, a_ref, h_ref, fr_ref, f_ref, xt_ref, gt_ref, g_ref, gram_a, gram_h = refs
    j = pl.program_id(0)
    seq = x_ref.shape[0] // n_samples
    half = seq // 2
    low, high = slice(0, half), slice(half, seq)

    @pl.when(j == 0)
    def _():
        gram_a[...] = jnp.zeros_like(gram_a)
        gram_h[...] = jnp.zeros_like(gram_h)
        if not first:
            for s in range(n_samples):
                rows = pl.ds(s * seq, seq)
                valid = lax.broadcasted_iota(jnp.int32, (seq, 1), 0) < len_ref[s]
                g_ref[rows, :] = jnp.where(valid, g_in[rows, :].astype(F32), 0.0).astype(BF16)

    width = xt_ref.shape[0]
    cols = pl.ds(pl.multiple_of(j * width, width), width)
    xt_ref[...] = x_ref[:, cols].T
    gt_ref[...] = g_ref[:, cols].T
    for s in range(n_samples):
        rows = pl.ds(s * seq, seq)
        if first:
            z = z_ref[rows, :].astype(F32)
        else:
            z = jnp.dot(x_ref[rows, :], wu_ref[0], preferred_element_type=F32).astype(BF16).astype(F32)
        u = dot_nt(g_ref[rows, :], wd_ref[0])
        cdf = normal_cdf(z)
        if first:
            a = a_ref[rows, :]
        else:
            a = (z * cdf).astype(BF16)
            a_ref[rows, :] = a
        h = (u * (cdf + z * jnp.exp(-0.5 * z * z) * 0.3989422804014327)).astype(BF16)
        h_ref[rows, :] = h
        gram_a[s, low, low] += dot_nt(a[low], a[low])
        gram_a[s, high, :] += dot_nt(a[high], a)
        gram_h[s, low, low] += dot_nt(h[low], h[low])
        gram_h[s, high, :] += dot_nt(h[high], h)

    @pl.when(j == pl.num_programs(0) - 1)
    def _():
        for s in range(n_samples):
            first_half, second_half = pl.ds(s * seq, half), pl.ds(s * seq + half, half)

            def paired(r, rr, c, cc):
                gg = dot_nt(g_ref[rr, :], g_ref[cc, :])
                xx = dot_nt(x_ref[rr, :], x_ref[cc, :])
                return gram_a[s, r, c] * gg + gram_h[s, r, c] * xx

            total = (paired(low, first_half, low, first_half) + paired(high, second_half, high, second_half)
                     + 2.0 * paired(high, second_half, low, first_half))
            norm_sq = jnp.sum(total, axis=(0, 1), keepdims=True)
            factor = jnp.minimum(1.0, clip_ref[0] / jnp.sqrt(norm_sq))
            f_ref[:, pl.ds(s * seq, seq)] = jnp.broadcast_to(factor, (1, seq))
            fr_ref[pl.ds(s * seq, seq), :] = jnp.broadcast_to(factor, (seq, 1))


def block_grad(layer, x_rows, g_rows, hidden, w_up, w_down, clip, lengths):
    n_rows, dim = x_rows.shape
    n_samples = lengths.shape[0]
    ff = w_up.shape[2]
    tile = 512
    steps = ff // tile
    seq = n_rows // n_samples
    col = pl.BlockSpec((n_rows, tile), lambda j: (0, j))
    whole = resident((n_rows, dim))
    wd_spec = pl.BlockSpec((1, tile, dim), lambda j: (layer, j, 0))
    big = jax.ShapeDtypeStruct((n_rows, ff), BF16)
    f_out = (jax.ShapeDtypeStruct((n_rows, 1), F32), jax.ShapeDtypeStruct((1, n_rows), F32))
    f_spec = (resident((n_rows, 1)), resident((1, n_rows)))
    turned, t_spec = jax.ShapeDtypeStruct((dim, n_rows), BF16), pl.BlockSpec((dim // steps, n_rows), lambda j: (j, 0))
    smem = pl.BlockSpec(memory_space=pltpu.SMEM)
    first = hidden is not None
    if first:
        in_specs = [smem, smem, whole, whole, col, col, wd_spec]
        args = (clip, lengths, x_rows, g_rows, hidden[0], hidden[1], w_down)
        out_shape, out_specs = (big, *f_out, turned, turned), (col, *f_spec, t_spec, t_spec)
    else:
        in_specs = [smem, smem, whole, whole, pl.BlockSpec((1, dim, tile), lambda j: (layer, 0, j)), wd_spec]
        args = (clip, lengths, x_rows, g_rows, w_up, w_down)
        out_shape = (big, big, *f_out, turned, turned, jax.ShapeDtypeStruct((n_rows, dim), BF16))
        out_specs = (col, col, *f_spec, t_spec, t_spec, whole)
    return pl.pallas_call(
        functools.partial(grad_kernel, first, n_samples), out_shape=out_shape, grid=(steps,), in_specs=in_specs, out_specs=out_specs,
        scratch_shapes=[pltpu.VMEM((n_samples, seq, seq), F32)] * 2, name='block_grad',
        cost_estimate=pl.CostEstimate(flops=((2 if first else 4) * dim + 3 * seq) * n_rows * ff, bytes_accessed=dim * ff * 4 + n_rows * ff * 4, transcendentals=2 * n_rows * ff),
        compiler_params=pltpu.CompilerParams(vmem_limit_bytes=60 * 1024 * 1024))(*args)


def axis_weight(axis):
    return 2 * (axis + 1) + 2 * (axis // 2)


def sums_kernel(shift, split, xt_hbm, h_hbm, a_hbm, gt_hbm, rowf, colf, r_hbm, *refs):
    late_hbm = refs[0] if split < CHUNKS else None
    (lt, slab, gpiece, clip, own, s0s, s0r, rc1, rc2, rc3, obuf,
     slab_sem, g_sem, o_sem, d_send, d_recv, sems_s, sems_r) = refs[-18:]
    me = lax.axis_index('data')
    core = me % 2
    partner = me + 1 - 2 * core

    def bit_peer(chunk, stage):
        axis = (chunk + shift + stage) % 3
        weight = axis_weight(axis)
        bit = (me // weight) % 2
        return bit, me + weight * (1 - 2 * bit)

    barrier = pltpu.get_barrier_semaphore()
    pl.semaphore_signal(barrier, inc=1, device_id=(partner,), device_id_type=MESH_ID)
    for axis in range(3):
        weight = axis_weight(axis)
        peer = me + weight * (1 - 2 * ((me // weight) % 2))
        pl.semaphore_signal(barrier, inc=1, device_id=(peer,), device_id_type=MESH_ID)

    def columns(half, chunk):
        return pl.ds(pl.multiple_of((half * PER_MAT + chunk % PER_MAT) * CW, CW), CW)

    def start_slab(half, chunk, buf):
        @pl.when(chunk < PER_MAT)
        def _():
            pltpu.make_async_copy(h_hbm.at[:, columns(half, chunk)], slab.at[buf], slab_sem.at[buf]).start()

        @pl.when(chunk >= PER_MAT)
        def _():
            pltpu.make_async_copy(a_hbm.at[:, columns(half, chunk)], slab.at[buf], slab_sem.at[buf]).start()

    def wait_slab(buf):
        pltpu.make_async_copy(h_hbm.at[:, pl.ds(0, CW)], slab.at[buf], slab_sem.at[buf]).wait()

    n_pieces = gt_hbm.shape[0] // CW
    x_copy = pltpu.make_async_copy(xt_hbm, lt.at[0], g_sem.at[1])

    def g_copy(piece):
        return pltpu.make_async_copy(gt_hbm.at[pl.ds(pl.multiple_of(piece * CW, CW), CW), :], gpiece, g_sem.at[0])

    start_slab(1 - core, 0, 0)
    x_copy.start()
    start_slab(core, 0, 2)
    pl.semaphore_wait(barrier, 4)
    x_copy.wait()

    def load_clip(chunk, buf):
        scale = jnp.where(chunk < PER_MAT, rowf[...], 1.0)
        clip[...] = (slab[buf].astype(F32) * scale).astype(BF16)

    def partner_chunk(chunk):
        buf = chunk % 2
        wait_slab(buf)
        load_clip(chunk, buf)

        @pl.when(chunk + 1 < CHUNKS)
        def _():
            start_slab(1 - core, chunk + 1, 1 - buf)

        mat = chunk // PER_MAT
        for q in range(4):
            rows = pl.ds(q * 512, 512)
            s0s[buf, rows, :] = jnp.dot(lt[mat, rows, :], clip[...], preferred_element_type=F32).astype(BF16)

    def d2d(chunk):
        buf = chunk % 2
        return pltpu.make_async_remote_copy(s0s.at[buf], s0r.at[buf], d_send.at[buf], d_recv.at[buf], device_id=(partner,), device_id_type=MESH_ID)

    def own_chunk(chunk):
        buf = 2 + chunk % 2
        wait_slab(buf)
        load_clip(chunk, buf)

        @pl.when(chunk + 1 < CHUNKS)
        def _():
            start_slab(core, chunk + 1, 5 - buf)

        d2d(chunk).wait()
        mat = chunk // PER_MAT
        for q in range(4):
            rows = pl.ds(q * 512, 512)
            part = jnp.dot(lt[mat, rows, :], clip[...], preferred_element_type=F32)
            own[chunk % OWN, rows, :] = (part + s0r[chunk % 2, rows, :].astype(F32)).astype(BF16)

    def kept_row(chunk, stage):
        row = 0
        for s in range(stage):
            bit, _ = bit_peer(chunk, s)
            row = row + bit * (1024 // (2 ** s))
        return row

    recv_bufs = (rc1, rc2, rc3)

    def stage_copy(chunk, stage):
        size = 1024 // (2 ** stage)
        bit, peer = bit_peer(chunk, stage)
        row = kept_row(chunk, stage) + (1 - bit) * size
        slot = chunk % RECV
        return pltpu.make_async_remote_copy(
            own.at[chunk % OWN, pl.ds(pl.multiple_of(row, CW), size), :], recv_bufs[stage].at[slot],
            sems_s.at[stage, slot], sems_r.at[stage, slot], device_id=(peer,), device_id_type=MESH_ID)

    def stage_sum(chunk, stage):
        size = 1024 // (2 ** stage)
        rows = pl.ds(pl.multiple_of(kept_row(chunk, stage + 1), CW), size)
        return rows, own[chunk % OWN, rows, :].astype(F32) + recv_bufs[stage][chunk % RECV].astype(F32)

    def start_out(chunk):
        @pl.when(chunk < split)
        def _():
            pltpu.make_async_copy(obuf.at[chunk % 2], r_hbm.at[chunk], o_sem.at[chunk % 2]).start()

        if split < CHUNKS:
            @pl.when(chunk >= split)
            def _():
                pltpu.make_async_copy(obuf.at[chunk % 2], late_hbm.at[chunk - split], o_sem.at[chunk % 2]).start()

    def wait_out(chunk):
        pltpu.make_async_copy(obuf.at[chunk % 2], r_hbm.at[0], o_sem.at[chunk % 2]).wait()

    partner_chunk(0)
    g_copy(0).start()
    d2d(0).start()

    def step(t, _):
        @pl.when(t >= LAG3)
        def _():
            chunk = t - LAG3
            stage_copy(chunk, 2).wait()
            _, total = stage_sum(chunk, 2)

            @pl.when(chunk >= 2)
            def _():
                wait_out(chunk - 2)

            @pl.when(chunk < PER_MAT)
            def _():
                obuf[chunk % 2] = total.astype(BF16)

            @pl.when(chunk >= PER_MAT)
            def _():
                obuf[chunk % 2] = total.T.astype(BF16)

            start_out(chunk)

        @pl.when((t >= LAG2) & (t < CHUNKS + LAG2))
        def _():
            chunk = t - LAG2
            stage_copy(chunk, 1).wait()
            rows, total = stage_sum(chunk, 1)
            own[chunk % OWN, rows, :] = total.astype(BF16)

        @pl.when((t >= LAG1) & (t < CHUNKS + LAG1))
        def _():
            chunk = t - LAG1
            stage_copy(chunk, 0).wait()
            rows, total = stage_sum(chunk, 0)
            own[chunk % OWN, rows, :] = total.astype(BF16)

        @pl.when((t >= 1) & (t < CHUNKS + 1))
        def _():
            stage_copy(t - 1, 0).start()

        @pl.when(t < n_pieces)
        def _():
            g_copy(t).wait()
            lt[1, pl.ds(pl.multiple_of(t * CW, CW), CW), :] = (gpiece[...].astype(F32) * colf[...]).astype(BF16)

            @pl.when(t + 1 < n_pieces)
            def _():
                g_copy(t + 1).start()

        @pl.when(t < CHUNKS - 1)
        def _():
            partner_chunk(t + 1)

        @pl.when(t < CHUNKS)
        def _():
            own_chunk(t)

        @pl.when(t < CHUNKS - 1)
        def _():
            d2d(t + 1).start()

        @pl.when((t >= LAG1) & (t < CHUNKS + LAG1))
        def _():
            stage_copy(t - LAG1, 1).start()

        @pl.when((t >= LAG2) & (t < CHUNKS + LAG2))
        def _():
            stage_copy(t - LAG2, 2).start()

        return 0

    lax.fori_loop(0, CHUNKS + LAG3, step, 0)
    wait_out(CHUNKS - 2)
    wait_out(CHUNKS - 1)


def block_sums(layer, split, x_turned, h_rows, a_rows, g_turned, factors):
    dim, n_rows = x_turned.shape
    scratch = [
        pltpu.VMEM((2, dim, n_rows), BF16), pltpu.VMEM((4, n_rows, CW), BF16), pltpu.VMEM((CW, n_rows), BF16), pltpu.VMEM((n_rows, CW), BF16),
        pltpu.VMEM((OWN, dim, CW), BF16), pltpu.VMEM((2, dim, CW), BF16), pltpu.VMEM((2, dim, CW), BF16),
        pltpu.VMEM((RECV, dim // 2, CW), BF16), pltpu.VMEM((RECV, dim // 4, CW), BF16), pltpu.VMEM((RECV, dim // 8, CW), BF16),
        pltpu.VMEM((2, CW, CW), BF16),
        pltpu.SemaphoreType.DMA((4,)), pltpu.SemaphoreType.DMA((2,)), pltpu.SemaphoreType.DMA((2,)),
        pltpu.SemaphoreType.DMA((2,)), pltpu.SemaphoreType.DMA((2,)), pltpu.SemaphoreType.DMA((3, RECV)), pltpu.SemaphoreType.DMA((3, RECV)),
    ]
    flops = 4 * n_rows * dim * h_rows.shape[1]
    sizes = (split, CHUNKS - split) if split < CHUNKS else (CHUNKS,)
    return pl.pallas_call(
        functools.partial(sums_kernel, 2 * layer, split),
        out_shape=tuple(jax.ShapeDtypeStruct((n, CW, CW), BF16) for n in sizes),
        in_specs=[ANY, ANY, ANY, ANY] + [pl.BlockSpec(memory_space=pltpu.VMEM)] * 2,
        out_specs=(ANY,) * len(sizes),
        scratch_shapes=scratch,
        compiler_params=pltpu.CompilerParams(collective_id=layer, has_side_effects=True, vmem_limit_bytes=60 * 1024 * 1024),
        cost_estimate=pl.CostEstimate(flops=flops, bytes_accessed=4 * n_rows * h_rows.shape[1], transcendentals=0),
        name=f'sums_{layer}',
    )(x_turned, h_rows, a_rows, g_turned, *factors)


def owner_of(chunk, piece, half, shift):
    color = (chunk + shift) % 3
    b1, b2, b3 = piece // 4, (piece // 2) % 2, piece % 2
    return b1 * axis_weight(color) + b2 * axis_weight((color + 1) % 3) + b3 * axis_weight((color + 2) % 3) + half


def finish_kernel(n_in, scale, *refs):
    pieces, noise, out = refs[:n_in], refs[n_in], refs[-1]
    across = out.shape[2] // CW
    for i in range(n_in):
        rows, cols = pl.ds(i // across * CW, CW), pl.ds(i % across * CW, CW)
        out[0, rows, cols] = (pieces[i][0, 0].astype(F32) + noise[0, rows, cols]) * scale


def finish_call(name, layer, grid, piece_specs, tile, gathered, noise, prev, batch_total):
    in_specs = piece_specs + [tile]
    args = [gathered] * len(piece_specs) + [noise]
    aliases = {}
    if prev is not None:
        in_specs.append(ANY)
        args.append(prev)
        aliases = {len(args) - 1: 0}
    steps = grid[0] * grid[1]
    size = steps * tile.block_shape[1] * tile.block_shape[2]
    return pl.pallas_call(
        functools.partial(finish_kernel, len(piece_specs), 1.0 / batch_total),
        out_shape=jax.ShapeDtypeStruct(noise.shape, F32), grid=grid, in_specs=in_specs, out_specs=tile,
        input_output_aliases=aliases, name=f'{name}_{layer}',
        cost_estimate=pl.CostEstimate(flops=size * 200, bytes_accessed=size * 10, transcendentals=0),
        compiler_params=pltpu.CompilerParams(vmem_limit_bytes=50 * 1024 * 1024))(*args)


def finish_up(layer, gathered, offset, start, n, noise, prev, batch_total):
    layers, dim, ff = noise.shape
    shift = 2 * layer

    def piece_spec(c):
        return pl.BlockSpec((1, 1, CW, CW), lambda i, k, c=c: (owner_of(start + c, i, k, shift), start - offset + c, 0, 0))

    per_half = ff // 2 // (n * CW)
    tile = pl.BlockSpec((1, CW, n * CW), lambda i, k: (layer, i, k * per_half + start // n))
    return finish_call('finish_up', layer, (dim // CW, 2), [piece_spec(c) for c in range(n)], tile, gathered, noise, prev, batch_total)


def finish_down(layer, gathered, offset, start, n, noise, prev, batch_total):
    layers, ff, dim = noise.shape
    shift, n_in = 2 * layer, dim // CW

    def piece_spec(d, i):
        def index(k, c):
            chunk = start + 2 * c + d
            return owner_of(chunk, i, k, shift), chunk - offset, 0, 0

        return pl.BlockSpec((1, 1, CW, CW), index)

    tile = pl.BlockSpec((1, 2 * CW, dim), lambda k, c: (layer, (k * PER_MAT + start - PER_MAT) // 2 + c, 0))
    specs = [piece_spec(d, i) for d in range(2) for i in range(n_in)]
    return finish_call('finish_down', layer, (2, n // 2), specs, tile, gathered, noise, prev, batch_total)


def per_device(x_in, dy_out, lengths, w_up, w_down, noise_up, noise_down, clip_norm, batch_total):
    n_samples, seq_len, dim = x_in.shape
    n_rows = n_samples * seq_len
    x_first = x_in.reshape(n_rows, dim)
    z_first, a_first, x_last = forward_block(0, x_first, w_up, w_down)
    a_last, h_last, row_f, col_f, x_turned, g_turned, g_last = block_grad(1, x_last, dy_out.reshape(n_rows, dim), None, w_up, w_down, clip_norm[1:], lengths)
    piece, = block_sums(1, CHUNKS, x_turned, h_last, a_last, g_turned, (row_f, col_f))
    gathered_last = lax.all_gather(piece, 'data')
    g_first = add_product(1, g_last, h_last, w_up, True)
    h_first, row_f, col_f, x_turned, g_turned = block_grad(0, x_first, g_first, (z_first, a_first), w_up, w_down, clip_norm[:1], lengths)
    pieces = block_sums(0, SPLIT, x_turned, h_first, a_first, g_turned, (row_f, col_f))
    part_a, part_b = [lax.all_gather(part, 'data') for part in pieces]
    grad_up = finish_up(1, gathered_last, 0, 0, PER_MAT, noise_up, None, batch_total)
    grad_down = finish_down(1, gathered_last, 0, PER_MAT, PER_MAT, noise_down, None, batch_total)
    grad_up, grad_down, part_a = lax.optimization_barrier((grad_up, grad_down, part_a))
    grad_up = finish_up(0, part_a, 0, 0, PER_MAT, noise_up, grad_up, batch_total)
    grad_down = finish_down(0, part_a, 0, PER_MAT, SPLIT - PER_MAT, noise_down, grad_down, batch_total)
    grad_up, grad_down, part_b = lax.optimization_barrier((grad_up, grad_down, part_b))
    grad_down = finish_down(0, part_b, SPLIT, SPLIT, CHUNKS - SPLIT, noise_down, grad_down, batch_total)
    return grad_up, grad_down


def solution(mesh):
    batch_spec = P('data', None, None)

    def grad_step(x_in, dy_out, lengths, w_up, w_down, noise_up, noise_down, clip_norm):
        device_fn = functools.partial(per_device, batch_total=x_in.shape[0])
        mapped = jax.shard_map(device_fn, mesh=mesh, in_specs=(batch_spec, batch_spec, P('data'), P(), P(), P(), P(), P()), out_specs=(P(), P()), check_vma=False)
        return mapped(x_in, dy_out, lengths, w_up, w_down, noise_up, noise_down, clip_norm)

    return grad_step
```

```python
import functools
import jax
import jax.numpy as jnp
from jax import lax
from jax.experimental import pallas as pl
from jax.experimental.pallas import tpu as pltpu
from jax.sharding import PartitionSpec as P

F32 = jnp.float32
BF16 = jnp.bfloat16
MESH_ID = pl.DeviceIdType.MESH
ANY = pl.BlockSpec(memory_space=pl.ANY)
CW = 256
PER_MAT = 16
CHUNKS = 2 * PER_MAT
SPLIT = 24
LAG1, LAG2, LAG3 = 4, 7, 10
RECV = 6
OWN = 10


def normal_cdf(z):
    return 0.5 * (1.0 + lax.erf(z * 0.7071067811865476))


def dot_nt(a, b):
    return lax.dot_general(a, b, (((1,), (1,)), ((), ())), preferred_element_type=F32)


def resident(shape):
    return pl.BlockSpec(shape, lambda j: (0, 0), pipeline_mode=pl.Buffered(buffer_count=1))


def add_grams(gram, s, block):
    half = block.shape[0] // 2
    low, high = slice(0, half), slice(half, 2 * half)
    gram[s, low, low] += dot_nt(block[low], block[low])
    gram[s, high, :] += dot_nt(block[high], block)


def write_factors(n_samples, clip, x_ref, g_ref, gram_a, gram_h, fr_ref, f_ref):
    seq = x_ref.shape[0] // n_samples
    half = seq // 2
    low, high = slice(0, half), slice(half, seq)
    for s in range(n_samples):
        first_half, second_half = pl.ds(s * seq, half), pl.ds(s * seq + half, half)

        def paired(r, rr, c, cc):
            gg = dot_nt(g_ref[rr, :], g_ref[cc, :])
            xx = dot_nt(x_ref[rr, :], x_ref[cc, :])
            return gram_a[s, r, c] * gg + gram_h[s, r, c] * xx

        total = (paired(low, first_half, low, first_half) + paired(high, second_half, high, second_half)
                 + 2.0 * paired(high, second_half, low, first_half))
        norm_sq = jnp.sum(total, axis=(0, 1), keepdims=True)
        factor = jnp.minimum(1.0, clip / jnp.sqrt(norm_sq))
        f_ref[:, pl.ds(s * seq, seq)] = jnp.broadcast_to(factor, (1, seq))
        fr_ref[pl.ds(s * seq, seq), :] = jnp.broadcast_to(factor, (seq, 1))


def turn_columns(j, x_ref, g_ref, xt_ref, gt_ref):
    width = xt_ref.shape[0]
    cols = pl.ds(pl.multiple_of(j * width, width), width)
    xt_ref[...] = x_ref[:, cols].T
    gt_ref[...] = g_ref[:, cols].T


def gelu_slope(z, cdf):
    return cdf + z * jnp.exp(-0.5 * z * z) * 0.3989422804014327


def first_kernel(n_samples, steps, clip_ref, len_ref, x_hbm, dy_hbm, wu_ref, wd_ref, z_ref, a_first, a_ref, h_ref, fr_ref, f_ref, xt_ref, gt_ref, g_ref,
                 x_ref, acc, gram_a, gram_h, sems):
    j = pl.program_id(0)
    n_rows = x_ref.shape[0]
    seq = n_rows // n_samples
    x_copy = pltpu.make_async_copy(x_hbm, x_ref, sems.at[0])
    g_copy = pltpu.make_async_copy(dy_hbm, g_ref, sems.at[1])

    @pl.when(j == 0)
    def _():
        x_copy.start()
        g_copy.start()
        x_copy.wait()
        acc[...] = x_ref[...].astype(F32)

    @pl.when(j < steps)
    def _():
        block = n_rows // 2
        for start in range(0, n_rows, block):
            rows = pl.ds(start, block)
            z = jnp.dot(x_ref[rows, :], wu_ref[0], preferred_element_type=F32).astype(BF16)
            z_ref[rows, :] = z
            zf = z.astype(F32)
            a = (zf * normal_cdf(zf)).astype(BF16)
            a_first[rows, :] = a
            acc[rows, :] += jnp.dot(a, wd_ref[0], preferred_element_type=F32)

    @pl.when(j == steps)
    def _():
        x_ref[...] = acc[...].astype(BF16)
        gram_a[...] = jnp.zeros_like(gram_a)
        gram_h[...] = jnp.zeros_like(gram_h)
        g_copy.wait()
        for s in range(n_samples):
            rows = pl.ds(s * seq, seq)
            valid = lax.broadcasted_iota(jnp.int32, (seq, 1), 0) < len_ref[s]
            g_ref[rows, :] = jnp.where(valid, g_ref[rows, :].astype(F32), 0.0).astype(BF16)

    @pl.when(j >= steps)
    def _():
        turn_columns(j - steps, x_ref, g_ref, xt_ref, gt_ref)
        for s in range(n_samples):
            rows = pl.ds(s * seq, seq)
            z = jnp.dot(x_ref[rows, :], wu_ref[0], preferred_element_type=F32).astype(BF16).astype(F32)
            u = dot_nt(g_ref[rows, :], wd_ref[0])
            cdf = normal_cdf(z)
            a = (z * cdf).astype(BF16)
            a_ref[rows, :] = a
            h = (u * gelu_slope(z, cdf)).astype(BF16)
            h_ref[rows, :] = h
            add_grams(gram_a, s, a)
            add_grams(gram_h, s, h)

    @pl.when(j == 2 * steps - 1)
    def _():
        write_factors(n_samples, clip_ref[1], x_ref, g_ref, gram_a, gram_h, fr_ref, f_ref)


def first_pass(x_rows, dy_rows, w_up, w_down, clip_norm, lengths):
    n_rows, dim = x_rows.shape
    n_samples = lengths.shape[0]
    ff = w_up.shape[2]
    tile = 512
    steps = ff // tile
    seq = n_rows // n_samples
    early = pl.BlockSpec((n_rows, tile), lambda j: (0, jnp.minimum(j, steps - 1)))
    late = pl.BlockSpec((n_rows, tile), lambda j: (0, jnp.maximum(j - steps, 0)))
    turned, t_spec = jax.ShapeDtypeStruct((dim, n_rows), BF16), pl.BlockSpec((dim // steps, n_rows), lambda j: (jnp.maximum(j - steps, 0), 0))
    big = jax.ShapeDtypeStruct((n_rows, ff), BF16)
    smem = pl.BlockSpec(memory_space=pltpu.SMEM)
    return pl.pallas_call(
        functools.partial(first_kernel, n_samples, steps), grid=(2 * steps,), name='first_pass',
        out_shape=(big, big, big, big, jax.ShapeDtypeStruct((n_rows, 1), F32), jax.ShapeDtypeStruct((1, n_rows), F32), turned, turned, jax.ShapeDtypeStruct((n_rows, dim), BF16)),
        in_specs=[smem, smem, ANY, ANY, pl.BlockSpec((1, dim, tile), lambda j: (j // steps, 0, j % steps)), pl.BlockSpec((1, tile, dim), lambda j: (j // steps, j % steps, 0))],
        out_specs=(early, early, late, late, resident((n_rows, 1)), resident((1, n_rows)), t_spec, t_spec, resident((n_rows, dim))),
        scratch_shapes=[pltpu.VMEM((n_rows, dim), BF16), pltpu.VMEM((n_rows, dim), F32)] + [pltpu.VMEM((n_samples, seq, seq), F32)] * 2 + [pltpu.SemaphoreType.DMA((2,))],
        cost_estimate=pl.CostEstimate(flops=(8 * dim + 3 * seq) * n_rows * ff, bytes_accessed=dim * ff * 8 + n_rows * ff * 8, transcendentals=3 * n_rows * ff),
        compiler_params=pltpu.CompilerParams(vmem_limit_bytes=63 * 1024 * 1024))(clip_norm, lengths, x_rows, dy_rows, w_up, w_down)


def add_kernel(transposed, a_ref, w_ref, x_ref, o_ref, acc):
    k = pl.program_id(1)

    @pl.when(k == 0)
    def _():
        acc[...] = x_ref[...].astype(F32)

    for start in range(0, a_ref.shape[0], 512):
        rows = pl.ds(start, 512)
        if transposed:
            acc[rows, :] += dot_nt(a_ref[rows, :], w_ref[0])
        else:
            acc[rows, :] += jnp.dot(a_ref[rows, :], w_ref[0], preferred_element_type=F32)

    @pl.when(k == pl.num_programs(1) - 1)
    def _():
        o_ref[...] = acc[...].astype(BF16)


def add_product(layer, x_rows, a_rows, weight, transposed):
    n_rows, dim = x_rows.shape
    ff = a_rows.shape[1]
    tn, tk = 1024, 2048
    if transposed:
        w_spec = pl.BlockSpec((1, tn, tk), lambda n, k: (layer, n, k))
    else:
        w_spec = pl.BlockSpec((1, tk, tn), lambda n, k: (layer, k, n))
    col = pl.BlockSpec((n_rows, tn), lambda n, k: (0, n))
    return pl.pallas_call(
        functools.partial(add_kernel, transposed), out_shape=jax.ShapeDtypeStruct((n_rows, dim), BF16), grid=(dim // tn, ff // tk),
        in_specs=[pl.BlockSpec((n_rows, tk), lambda n, k: (0, k)), w_spec, col],
        out_specs=col, scratch_shapes=[pltpu.VMEM((n_rows, tn), F32)], name='add_product',
        cost_estimate=pl.CostEstimate(flops=2 * n_rows * dim * ff, bytes_accessed=dim * ff * 2 + n_rows * ff * 4, transcendentals=0),
        compiler_params=pltpu.CompilerParams(vmem_limit_bytes=60 * 1024 * 1024))(a_rows, weight, x_rows)


def grad_kernel(n_samples, clip_ref, x_ref, g_ref, z_ref, a_ref, wd_ref, h_ref, fr_ref, f_ref, xt_ref, gt_ref, gram_a, gram_h):
    j = pl.program_id(0)
    seq = x_ref.shape[0] // n_samples

    @pl.when(j == 0)
    def _():
        gram_a[...] = jnp.zeros_like(gram_a)
        gram_h[...] = jnp.zeros_like(gram_h)

    turn_columns(j, x_ref, g_ref, xt_ref, gt_ref)
    for s in range(n_samples):
        rows = pl.ds(s * seq, seq)
        z = z_ref[rows, :].astype(F32)
        u = dot_nt(g_ref[rows, :], wd_ref[0])
        h = (u * gelu_slope(z, normal_cdf(z))).astype(BF16)
        h_ref[rows, :] = h
        add_grams(gram_a, s, a_ref[rows, :])
        add_grams(gram_h, s, h)

    @pl.when(j == pl.num_programs(0) - 1)
    def _():
        write_factors(n_samples, clip_ref[0], x_ref, g_ref, gram_a, gram_h, fr_ref, f_ref)


def block_grad(x_rows, g_rows, z_rows, a_rows, w_down, clip_norm, n_samples):
    n_rows, dim = x_rows.shape
    ff = z_rows.shape[1]
    tile = 512
    steps = ff // tile
    seq = n_rows // n_samples
    col = pl.BlockSpec((n_rows, tile), lambda j: (0, j))
    whole = resident((n_rows, dim))
    turned, t_spec = jax.ShapeDtypeStruct((dim, n_rows), BF16), pl.BlockSpec((dim // steps, n_rows), lambda j: (j, 0))
    return pl.pallas_call(
        functools.partial(grad_kernel, n_samples), grid=(steps,), name='block_grad',
        out_shape=(jax.ShapeDtypeStruct((n_rows, ff), BF16), jax.ShapeDtypeStruct((n_rows, 1), F32), jax.ShapeDtypeStruct((1, n_rows), F32), turned, turned),
        in_specs=[pl.BlockSpec(memory_space=pltpu.SMEM), whole, whole, col, col, pl.BlockSpec((1, tile, dim), lambda j: (0, j, 0))],
        out_specs=(col, resident((n_rows, 1)), resident((1, n_rows)), t_spec, t_spec),
        scratch_shapes=[pltpu.VMEM((n_samples, seq, seq), F32)] * 2,
        cost_estimate=pl.CostEstimate(flops=(2 * dim + 3 * seq) * n_rows * ff, bytes_accessed=dim * ff * 2 + n_rows * ff * 6, transcendentals=2 * n_rows * ff),
        compiler_params=pltpu.CompilerParams(vmem_limit_bytes=60 * 1024 * 1024))(clip_norm, x_rows, g_rows, z_rows, a_rows, w_down)


def axis_weight(axis):
    return 2 * (axis + 1) + 2 * (axis // 2)


def sums_kernel(shift, split, xt_hbm, h_hbm, a_hbm, gt_hbm, rowf, colf, r_hbm, *refs):
    late_hbm = refs[0] if split < CHUNKS else None
    (lt, slab, gpiece, clip, own, s0s, s0r, rc1, rc2, rc3, obuf,
     slab_sem, g_sem, o_sem, d_send, d_recv, sems_s, sems_r) = refs[-18:]
    me = lax.axis_index('data')
    core = me % 2
    partner = me + 1 - 2 * core

    def bit_peer(chunk, stage):
        axis = (chunk + shift + stage) % 3
        weight = axis_weight(axis)
        bit = (me // weight) % 2
        return bit, me + weight * (1 - 2 * bit)

    barrier = pltpu.get_barrier_semaphore()
    pl.semaphore_signal(barrier, inc=1, device_id=(partner,), device_id_type=MESH_ID)
    for axis in range(3):
        weight = axis_weight(axis)
        peer = me + weight * (1 - 2 * ((me // weight) % 2))
        pl.semaphore_signal(barrier, inc=1, device_id=(peer,), device_id_type=MESH_ID)

    def columns(half, chunk):
        return pl.ds(pl.multiple_of((half * PER_MAT + chunk % PER_MAT) * CW, CW), CW)

    def start_slab(half, chunk, buf):
        @pl.when(chunk < PER_MAT)
        def _():
            pltpu.make_async_copy(h_hbm.at[:, columns(half, chunk)], slab.at[buf], slab_sem.at[buf]).start()

        @pl.when(chunk >= PER_MAT)
        def _():
            pltpu.make_async_copy(a_hbm.at[:, columns(half, chunk)], slab.at[buf], slab_sem.at[buf]).start()

    def wait_slab(buf):
        pltpu.make_async_copy(h_hbm.at[:, pl.ds(0, CW)], slab.at[buf], slab_sem.at[buf]).wait()

    n_pieces = gt_hbm.shape[0] // CW

    def x_copy(q):
        rows = pl.ds(q * 512, 512)
        return pltpu.make_async_copy(xt_hbm.at[rows, :], lt.at[0, rows, :], g_sem.at[1 + q])

    def g_copy(piece):
        return pltpu.make_async_copy(gt_hbm.at[pl.ds(pl.multiple_of(piece * CW, CW), CW), :], gpiece, g_sem.at[0])

    start_slab(1 - core, 0, 0)
    for q in range(4):
        x_copy(q).start()
    start_slab(core, 0, 2)

    def load_clip(chunk, buf):
        scale = jnp.where(chunk < PER_MAT, rowf[...], 1.0)
        clip[...] = (slab[buf].astype(F32) * scale).astype(BF16)

    def partner_chunk(chunk, opening=False):
        buf = chunk % 2
        wait_slab(buf)
        load_clip(chunk, buf)

        @pl.when(chunk + 1 < CHUNKS)
        def _():
            start_slab(1 - core, chunk + 1, 1 - buf)

        mat = chunk // PER_MAT
        for q in range(4):
            rows = pl.ds(q * 512, 512)
            if opening:
                x_copy(q).wait()
            s0s[buf, rows, :] = jnp.dot(lt[mat, rows, :], clip[...], preferred_element_type=F32).astype(BF16)

    def d2d(chunk):
        buf = chunk % 2
        return pltpu.make_async_remote_copy(s0s.at[buf], s0r.at[buf], d_send.at[buf], d_recv.at[buf], device_id=(partner,), device_id_type=MESH_ID)

    def own_chunk(chunk):
        buf = 2 + chunk % 2
        wait_slab(buf)
        load_clip(chunk, buf)

        @pl.when(chunk + 1 < CHUNKS)
        def _():
            start_slab(core, chunk + 1, 5 - buf)

        d2d(chunk).wait()
        mat = chunk // PER_MAT
        for q in range(4):
            rows = pl.ds(q * 512, 512)
            part = jnp.dot(lt[mat, rows, :], clip[...], preferred_element_type=F32)
            own[chunk % OWN, rows, :] = (part + s0r[chunk % 2, rows, :].astype(F32)).astype(BF16)

    def kept_row(chunk, stage):
        row = 0
        for s in range(stage):
            bit, _ = bit_peer(chunk, s)
            row = row + bit * (1024 // (2 ** s))
        return row

    recv_bufs = (rc1, rc2, rc3)

    def stage_copy(chunk, stage):
        size = 1024 // (2 ** stage)
        bit, peer = bit_peer(chunk, stage)
        row = kept_row(chunk, stage) + (1 - bit) * size
        slot = chunk % RECV
        return pltpu.make_async_remote_copy(
            own.at[chunk % OWN, pl.ds(pl.multiple_of(row, CW), size), :], recv_bufs[stage].at[slot],
            sems_s.at[stage, slot], sems_r.at[stage, slot], device_id=(peer,), device_id_type=MESH_ID)

    def stage_sum(chunk, stage):
        size = 1024 // (2 ** stage)
        rows = pl.ds(pl.multiple_of(kept_row(chunk, stage + 1), CW), size)
        return rows, own[chunk % OWN, rows, :].astype(F32) + recv_bufs[stage][chunk % RECV].astype(F32)

    def start_out(chunk):
        @pl.when(chunk < split)
        def _():
            pltpu.make_async_copy(obuf.at[chunk % 2], r_hbm.at[chunk], o_sem.at[chunk % 2]).start()

        if split < CHUNKS:
            @pl.when(chunk >= split)
            def _():
                pltpu.make_async_copy(obuf.at[chunk % 2], late_hbm.at[chunk - split], o_sem.at[chunk % 2]).start()

    def wait_out(chunk):
        pltpu.make_async_copy(obuf.at[chunk % 2], r_hbm.at[0], o_sem.at[chunk % 2]).wait()

    partner_chunk(0, True)
    g_copy(0).start()
    pl.semaphore_wait(barrier, 4)
    d2d(0).start()

    def step(t, _):
        @pl.when(t >= LAG3)
        def _():
            chunk = t - LAG3
            stage_copy(chunk, 2).wait()
            _, total = stage_sum(chunk, 2)

            @pl.when(chunk >= 2)
            def _():
                wait_out(chunk - 2)

            @pl.when(chunk < PER_MAT)
            def _():
                obuf[chunk % 2] = total.astype(BF16)

            @pl.when(chunk >= PER_MAT)
            def _():
                obuf[chunk % 2] = total.T.astype(BF16)

            start_out(chunk)

        @pl.when((t >= LAG2) & (t < CHUNKS + LAG2))
        def _():
            chunk = t - LAG2
            stage_copy(chunk, 1).wait()
            rows, total = stage_sum(chunk, 1)
            own[chunk % OWN, rows, :] = total.astype(BF16)

        @pl.when((t >= LAG1) & (t < CHUNKS + LAG1))
        def _():
            chunk = t - LAG1
            stage_copy(chunk, 0).wait()
            rows, total = stage_sum(chunk, 0)
            own[chunk % OWN, rows, :] = total.astype(BF16)

        @pl.when((t >= 1) & (t < CHUNKS + 1))
        def _():
            stage_copy(t - 1, 0).start()

        @pl.when(t < n_pieces)
        def _():
            g_copy(t).wait()
            lt[1, pl.ds(pl.multiple_of(t * CW, CW), CW), :] = (gpiece[...].astype(F32) * colf[...]).astype(BF16)

            @pl.when(t + 1 < n_pieces)
            def _():
                g_copy(t + 1).start()

        @pl.when(t < CHUNKS - 1)
        def _():
            partner_chunk(t + 1)

        @pl.when(t < CHUNKS)
        def _():
            own_chunk(t)

        @pl.when(t < CHUNKS - 1)
        def _():
            d2d(t + 1).start()

        @pl.when((t >= LAG1) & (t < CHUNKS + LAG1))
        def _():
            stage_copy(t - LAG1, 1).start()

        @pl.when((t >= LAG2) & (t < CHUNKS + LAG2))
        def _():
            stage_copy(t - LAG2, 2).start()

        return 0

    lax.fori_loop(0, CHUNKS + LAG3, step, 0)
    wait_out(CHUNKS - 2)
    wait_out(CHUNKS - 1)


def block_sums(layer, split, x_turned, h_rows, a_rows, g_turned, factors):
    dim, n_rows = x_turned.shape
    scratch = [
        pltpu.VMEM((2, dim, n_rows), BF16), pltpu.VMEM((4, n_rows, CW), BF16), pltpu.VMEM((CW, n_rows), BF16), pltpu.VMEM((n_rows, CW), BF16),
        pltpu.VMEM((OWN, dim, CW), BF16), pltpu.VMEM((2, dim, CW), BF16), pltpu.VMEM((2, dim, CW), BF16),
        pltpu.VMEM((RECV, dim // 2, CW), BF16), pltpu.VMEM((RECV, dim // 4, CW), BF16), pltpu.VMEM((RECV, dim // 8, CW), BF16),
        pltpu.VMEM((2, CW, CW), BF16),
        pltpu.SemaphoreType.DMA((4,)), pltpu.SemaphoreType.DMA((5,)), pltpu.SemaphoreType.DMA((2,)),
        pltpu.SemaphoreType.DMA((2,)), pltpu.SemaphoreType.DMA((2,)), pltpu.SemaphoreType.DMA((3, RECV)), pltpu.SemaphoreType.DMA((3, RECV)),
    ]
    flops = 4 * n_rows * dim * h_rows.shape[1]
    sizes = (split, CHUNKS - split) if split < CHUNKS else (CHUNKS,)
    return pl.pallas_call(
        functools.partial(sums_kernel, 2 * layer, split),
        out_shape=tuple(jax.ShapeDtypeStruct((n, CW, CW), BF16) for n in sizes),
        in_specs=[ANY, ANY, ANY, ANY] + [pl.BlockSpec(memory_space=pltpu.VMEM)] * 2,
        out_specs=(ANY,) * len(sizes),
        scratch_shapes=scratch,
        compiler_params=pltpu.CompilerParams(collective_id=layer, has_side_effects=True, vmem_limit_bytes=60 * 1024 * 1024),
        cost_estimate=pl.CostEstimate(flops=flops, bytes_accessed=4 * n_rows * h_rows.shape[1], transcendentals=0),
        name=f'sums_{layer}',
    )(x_turned, h_rows, a_rows, g_turned, *factors)


def owner_of(chunk, piece, half, shift):
    color = (chunk + shift) % 3
    b1, b2, b3 = piece // 4, (piece // 2) % 2, piece % 2
    return b1 * axis_weight(color) + b2 * axis_weight((color + 1) % 3) + b3 * axis_weight((color + 2) % 3) + half


def finish_kernel(n_in, scale, *refs):
    pieces, noise, out = refs[:n_in], refs[n_in], refs[-1]
    across = out.shape[2] // CW
    for i in range(n_in):
        rows, cols = pl.ds(i // across * CW, CW), pl.ds(i % across * CW, CW)
        out[0, rows, cols] = (pieces[i][0, 0].astype(F32) + noise[0, rows, cols]) * scale


def finish_call(name, layer, grid, piece_specs, tile, gathered, noise, prev, batch_total):
    in_specs = piece_specs + [tile]
    args = [gathered] * len(piece_specs) + [noise]
    aliases = {}
    if prev is not None:
        in_specs.append(ANY)
        args.append(prev)
        aliases = {len(args) - 1: 0}
    steps = grid[0] * grid[1]
    size = steps * tile.block_shape[1] * tile.block_shape[2]
    return pl.pallas_call(
        functools.partial(finish_kernel, len(piece_specs), 1.0 / batch_total),
        out_shape=jax.ShapeDtypeStruct(noise.shape, F32), grid=grid, in_specs=in_specs, out_specs=tile,
        input_output_aliases=aliases, name=f'{name}_{layer}',
        cost_estimate=pl.CostEstimate(flops=size * 200, bytes_accessed=size * 10, transcendentals=0),
        compiler_params=pltpu.CompilerParams(vmem_limit_bytes=50 * 1024 * 1024))(*args)


def finish_up(layer, gathered, offset, start, n, noise, prev, batch_total):
    layers, dim, ff = noise.shape
    shift = 2 * layer

    def piece_spec(c):
        return pl.BlockSpec((1, 1, CW, CW), lambda i, k, c=c: (owner_of(start + c, i, k, shift), start - offset + c, 0, 0))

    per_half = ff // 2 // (n * CW)
    tile = pl.BlockSpec((1, CW, n * CW), lambda i, k: (layer, i, k * per_half + start // n))
    return finish_call('finish_up', layer, (dim // CW, 2), [piece_spec(c) for c in range(n)], tile, gathered, noise, prev, batch_total)


def finish_down(layer, gathered, offset, start, n, noise, prev, batch_total):
    layers, ff, dim = noise.shape
    shift, n_in = 2 * layer, dim // CW

    def piece_spec(d, i):
        def index(k, c):
            chunk = start + 2 * c + d
            return owner_of(chunk, i, k, shift), chunk - offset, 0, 0

        return pl.BlockSpec((1, 1, CW, CW), index)

    tile = pl.BlockSpec((1, 2 * CW, dim), lambda k, c: (layer, (k * PER_MAT + start - PER_MAT) // 2 + c, 0))
    specs = [piece_spec(d, i) for d in range(2) for i in range(n_in)]
    return finish_call('finish_down', layer, (2, n // 2), specs, tile, gathered, noise, prev, batch_total)


def per_device(x_in, dy_out, lengths, w_up, w_down, noise_up, noise_down, clip_norm, batch_total):
    n_samples, seq_len, dim = x_in.shape
    n_rows = n_samples * seq_len
    x_first = x_in.reshape(n_rows, dim)
    z_first, a_first, a_last, h_last, row_f, col_f, x_turned, g_turned, g_last = first_pass(x_first, dy_out.reshape(n_rows, dim), w_up, w_down, clip_norm, lengths)
    piece, = block_sums(1, CHUNKS, x_turned, h_last, a_last, g_turned, (row_f, col_f))
    gathered_last = lax.all_gather(piece, 'data')
    g_first = add_product(1, g_last, h_last, w_up, True)
    h_first, row_f, col_f, x_turned, g_turned = block_grad(x_first, g_first, z_first, a_first, w_down, clip_norm, n_samples)
    pieces = block_sums(0, SPLIT, x_turned, h_first, a_first, g_turned, (row_f, col_f))
    part_a, part_b = [lax.all_gather(part, 'data') for part in pieces]
    grad_up = finish_up(1, gathered_last, 0, 0, PER_MAT, noise_up, None, batch_total)
    grad_down = finish_down(1, gathered_last, 0, PER_MAT, PER_MAT, noise_down, None, batch_total)
    grad_up, grad_down, part_a = lax.optimization_barrier((grad_up, grad_down, part_a))
    grad_up = finish_up(0, part_a, 0, 0, PER_MAT, noise_up, grad_up, batch_total)
    grad_down = finish_down(0, part_a, 0, PER_MAT, SPLIT - PER_MAT, noise_down, grad_down, batch_total)
    grad_up, grad_down, part_b = lax.optimization_barrier((grad_up, grad_down, part_b))
    grad_down = finish_down(0, part_b, SPLIT, SPLIT, CHUNKS - SPLIT, noise_down, grad_down, batch_total)
    return grad_up, grad_down


def solution(mesh):
    batch_spec = P('data', None, None)

    def grad_step(x_in, dy_out, lengths, w_up, w_down, noise_up, noise_down, clip_norm):
        device_fn = functools.partial(per_device, batch_total=x_in.shape[0])
        mapped = jax.shard_map(device_fn, mesh=mesh, in_specs=(batch_spec, batch_spec, P('data'), P(), P(), P(), P(), P()), out_specs=(P(), P()), check_vma=False)
        return mapped(x_in, dy_out, lengths, w_up, w_down, noise_up, noise_down, clip_norm)

    return grad_step
```

```python
import functools
import jax
import jax.numpy as jnp
from jax import lax
from jax.experimental import pallas as pl
from jax.experimental.pallas import tpu as pltpu
from jax.sharding import PartitionSpec as P

F32 = jnp.float32
BF16 = jnp.bfloat16
MESH_ID = pl.DeviceIdType.MESH
ANY = pl.BlockSpec(memory_space=pl.ANY)
CW = 256
PER_MAT = 16
CHUNKS = 2 * PER_MAT
BOUNDS = (4, 24, 32)
LAG1, LAG2, LAG3 = 4, 7, 10
RECV = 6
OWN = 10


def normal_cdf(z):
    return 0.5 * (1.0 + lax.erf(z * 0.7071067811865476))


def dot_nt(a, b):
    return lax.dot_general(a, b, (((1,), (1,)), ((), ())), preferred_element_type=F32)


def resident(shape):
    return pl.BlockSpec(shape, lambda j: (0, 0), pipeline_mode=pl.Buffered(buffer_count=1))


def add_grams(gram, s, block):
    half = block.shape[0] // 2
    low, high = slice(0, half), slice(half, 2 * half)
    gram[s, low, low] += dot_nt(block[low], block[low])
    gram[s, high, :] += dot_nt(block[high], block)


def write_factors(n_samples, clip, x_ref, g_ref, gram_a, gram_h, fr_ref, f_ref):
    seq = x_ref.shape[0] // n_samples
    half = seq // 2
    low, high = slice(0, half), slice(half, seq)
    for s in range(n_samples):
        first_half, second_half = pl.ds(s * seq, half), pl.ds(s * seq + half, half)

        def paired(r, rr, c, cc):
            gg = dot_nt(g_ref[rr, :], g_ref[cc, :])
            xx = dot_nt(x_ref[rr, :], x_ref[cc, :])
            return gram_a[s, r, c] * gg + gram_h[s, r, c] * xx

        total = (paired(low, first_half, low, first_half) + paired(high, second_half, high, second_half)
                 + 2.0 * paired(high, second_half, low, first_half))
        norm_sq = jnp.sum(total, axis=(0, 1), keepdims=True)
        factor = jnp.minimum(1.0, clip / jnp.sqrt(norm_sq))
        f_ref[:, pl.ds(s * seq, seq)] = jnp.broadcast_to(factor, (1, seq))
        fr_ref[pl.ds(s * seq, seq), :] = jnp.broadcast_to(factor, (seq, 1))


def turn_columns(j, x_ref, g_ref, xt_ref, gt_ref):
    width = xt_ref.shape[0]
    cols = pl.ds(pl.multiple_of(j * width, width), width)
    xt_ref[...] = x_ref[:, cols].T
    gt_ref[...] = g_ref[:, cols].T


def gelu_slope(z, cdf):
    return cdf + z * jnp.exp(-0.5 * z * z) * 0.3989422804014327


def first_kernel(n_samples, steps, clip_ref, len_ref, x_hbm, dy_hbm, wu_ref, wd_ref, z_ref, a_first, a_ref, h_ref, fr_ref, f_ref, xt_ref, gt_ref, g_ref,
                 x_ref, acc, gram_a, gram_h, sems):
    j = pl.program_id(0)
    n_rows = x_ref.shape[0]
    seq = n_rows // n_samples
    x_copy = pltpu.make_async_copy(x_hbm, x_ref, sems.at[0])
    g_copy = pltpu.make_async_copy(dy_hbm, g_ref, sems.at[1])

    @pl.when(j == 0)
    def _():
        x_copy.start()
        g_copy.start()
        x_copy.wait()
        acc[...] = x_ref[...].astype(F32)

    @pl.when(j < steps)
    def _():
        block = n_rows // 2
        for start in range(0, n_rows, block):
            rows = pl.ds(start, block)
            z = jnp.dot(x_ref[rows, :], wu_ref[0], preferred_element_type=F32).astype(BF16)
            z_ref[rows, :] = z
            zf = z.astype(F32)
            a = (zf * normal_cdf(zf)).astype(BF16)
            a_first[rows, :] = a
            acc[rows, :] += jnp.dot(a, wd_ref[0], preferred_element_type=F32)

    @pl.when(j == steps)
    def _():
        x_ref[...] = acc[...].astype(BF16)
        gram_a[...] = jnp.zeros_like(gram_a)
        gram_h[...] = jnp.zeros_like(gram_h)
        g_copy.wait()
        for s in range(n_samples):
            rows = pl.ds(s * seq, seq)
            valid = lax.broadcasted_iota(jnp.int32, (seq, 1), 0) < len_ref[s]
            g_ref[rows, :] = jnp.where(valid, g_ref[rows, :].astype(F32), 0.0).astype(BF16)

    @pl.when(j >= steps)
    def _():
        turn_columns(j - steps, x_ref, g_ref, xt_ref, gt_ref)
        for s in range(n_samples):
            rows = pl.ds(s * seq, seq)
            z = jnp.dot(x_ref[rows, :], wu_ref[0], preferred_element_type=F32).astype(BF16).astype(F32)
            u = dot_nt(g_ref[rows, :], wd_ref[0])
            cdf = normal_cdf(z)
            a = (z * cdf).astype(BF16)
            a_ref[rows, :] = a
            h = (u * gelu_slope(z, cdf)).astype(BF16)
            h_ref[rows, :] = h
            add_grams(gram_a, s, a)
            add_grams(gram_h, s, h)

    @pl.when(j == 2 * steps - 1)
    def _():
        write_factors(n_samples, clip_ref[1], x_ref, g_ref, gram_a, gram_h, fr_ref, f_ref)


def first_pass(x_rows, dy_rows, w_up, w_down, clip_norm, lengths):
    n_rows, dim = x_rows.shape
    n_samples = lengths.shape[0]
    ff = w_up.shape[2]
    tile = 512
    steps = ff // tile
    seq = n_rows // n_samples
    early = pl.BlockSpec((n_rows, tile), lambda j: (0, jnp.minimum(j, steps - 1)))
    late = pl.BlockSpec((n_rows, tile), lambda j: (0, jnp.maximum(j - steps, 0)))
    turned, t_spec = jax.ShapeDtypeStruct((dim, n_rows), BF16), pl.BlockSpec((dim // steps, n_rows), lambda j: (jnp.maximum(j - steps, 0), 0))
    big = jax.ShapeDtypeStruct((n_rows, ff), BF16)
    smem = pl.BlockSpec(memory_space=pltpu.SMEM)
    return pl.pallas_call(
        functools.partial(first_kernel, n_samples, steps), grid=(2 * steps,), name='first_pass',
        out_shape=(big, big, big, big, jax.ShapeDtypeStruct((n_rows, 1), F32), jax.ShapeDtypeStruct((1, n_rows), F32), turned, turned, jax.ShapeDtypeStruct((n_rows, dim), BF16)),
        in_specs=[smem, smem, ANY, ANY, pl.BlockSpec((1, dim, tile), lambda j: (j // steps, 0, j % steps)), pl.BlockSpec((1, tile, dim), lambda j: (j // steps, j % steps, 0))],
        out_specs=(early, early, late, late, resident((n_rows, 1)), resident((1, n_rows)), t_spec, t_spec, resident((n_rows, dim))),
        scratch_shapes=[pltpu.VMEM((n_rows, dim), BF16), pltpu.VMEM((n_rows, dim), F32)] + [pltpu.VMEM((n_samples, seq, seq), F32)] * 2 + [pltpu.SemaphoreType.DMA((2,))],
        cost_estimate=pl.CostEstimate(flops=(8 * dim + 3 * seq) * n_rows * ff, bytes_accessed=dim * ff * 8 + n_rows * ff * 8, transcendentals=3 * n_rows * ff),
        compiler_params=pltpu.CompilerParams(vmem_limit_bytes=63 * 1024 * 1024))(clip_norm, lengths, x_rows, dy_rows, w_up, w_down)


def add_kernel(transposed, a_ref, w_ref, x_ref, o_ref, acc):
    k = pl.program_id(1)

    @pl.when(k == 0)
    def _():
        acc[...] = x_ref[...].astype(F32)

    for start in range(0, a_ref.shape[0], 512):
        rows = pl.ds(start, 512)
        if transposed:
            acc[rows, :] += dot_nt(a_ref[rows, :], w_ref[0])
        else:
            acc[rows, :] += jnp.dot(a_ref[rows, :], w_ref[0], preferred_element_type=F32)

    @pl.when(k == pl.num_programs(1) - 1)
    def _():
        o_ref[...] = acc[...].astype(BF16)


def add_product(layer, x_rows, a_rows, weight, transposed):
    n_rows, dim = x_rows.shape
    ff = a_rows.shape[1]
    tn, tk = 1024, 2048
    if transposed:
        w_spec = pl.BlockSpec((1, tn, tk), lambda n, k: (layer, n, k))
    else:
        w_spec = pl.BlockSpec((1, tk, tn), lambda n, k: (layer, k, n))
    col = pl.BlockSpec((n_rows, tn), lambda n, k: (0, n))
    return pl.pallas_call(
        functools.partial(add_kernel, transposed), out_shape=jax.ShapeDtypeStruct((n_rows, dim), BF16), grid=(dim // tn, ff // tk),
        in_specs=[pl.BlockSpec((n_rows, tk), lambda n, k: (0, k)), w_spec, col],
        out_specs=col, scratch_shapes=[pltpu.VMEM((n_rows, tn), F32)], name='add_product',
        cost_estimate=pl.CostEstimate(flops=2 * n_rows * dim * ff, bytes_accessed=dim * ff * 2 + n_rows * ff * 4, transcendentals=0),
        compiler_params=pltpu.CompilerParams(vmem_limit_bytes=60 * 1024 * 1024))(a_rows, weight, x_rows)


def grad_kernel(n_samples, clip_ref, x_ref, g_ref, z_ref, a_ref, wd_ref, h_ref, fr_ref, f_ref, xt_ref, gt_ref, gram_a, gram_h):
    j = pl.program_id(0)
    seq = x_ref.shape[0] // n_samples

    @pl.when(j == 0)
    def _():
        gram_a[...] = jnp.zeros_like(gram_a)
        gram_h[...] = jnp.zeros_like(gram_h)

    turn_columns(j, x_ref, g_ref, xt_ref, gt_ref)
    for s in range(n_samples):
        rows = pl.ds(s * seq, seq)
        z = z_ref[rows, :].astype(F32)
        u = dot_nt(g_ref[rows, :], wd_ref[0])
        h = (u * gelu_slope(z, normal_cdf(z))).astype(BF16)
        h_ref[rows, :] = h
        add_grams(gram_a, s, a_ref[rows, :])
        add_grams(gram_h, s, h)

    @pl.when(j == pl.num_programs(0) - 1)
    def _():
        write_factors(n_samples, clip_ref[0], x_ref, g_ref, gram_a, gram_h, fr_ref, f_ref)


def block_grad(x_rows, g_rows, z_rows, a_rows, w_down, clip_norm, n_samples):
    n_rows, dim = x_rows.shape
    ff = z_rows.shape[1]
    tile = 512
    steps = ff // tile
    seq = n_rows // n_samples
    col = pl.BlockSpec((n_rows, tile), lambda j: (0, j))
    whole = resident((n_rows, dim))
    turned, t_spec = jax.ShapeDtypeStruct((dim, n_rows), BF16), pl.BlockSpec((dim // steps, n_rows), lambda j: (j, 0))
    return pl.pallas_call(
        functools.partial(grad_kernel, n_samples), grid=(steps,), name='block_grad',
        out_shape=(jax.ShapeDtypeStruct((n_rows, ff), BF16), jax.ShapeDtypeStruct((n_rows, 1), F32), jax.ShapeDtypeStruct((1, n_rows), F32), turned, turned),
        in_specs=[pl.BlockSpec(memory_space=pltpu.SMEM), whole, whole, col, col, pl.BlockSpec((1, tile, dim), lambda j: (0, j, 0))],
        out_specs=(col, resident((n_rows, 1)), resident((1, n_rows)), t_spec, t_spec),
        scratch_shapes=[pltpu.VMEM((n_samples, seq, seq), F32)] * 2,
        cost_estimate=pl.CostEstimate(flops=(2 * dim + 3 * seq) * n_rows * ff, bytes_accessed=dim * ff * 2 + n_rows * ff * 6, transcendentals=2 * n_rows * ff),
        compiler_params=pltpu.CompilerParams(vmem_limit_bytes=60 * 1024 * 1024))(clip_norm, x_rows, g_rows, z_rows, a_rows, w_down)


def axis_weight(axis):
    return 2 * (axis + 1) + 2 * (axis // 2)


def sums_kernel(shift, bounds, xt_hbm, h_hbm, a_hbm, gt_hbm, rowf, colf, *refs):
    outs = refs[:len(bounds)]
    (lt, slab, gpiece, clip, own, s0s, s0r, rc1, rc2, rc3, obuf,
     slab_sem, g_sem, o_sem, d_send, d_recv, sems_s, sems_r) = refs[-18:]
    me = lax.axis_index('data')
    core = me % 2
    partner = me + 1 - 2 * core

    def bit_peer(chunk, stage):
        axis = (chunk + shift + stage) % 3
        weight = axis_weight(axis)
        bit = (me // weight) % 2
        return bit, me + weight * (1 - 2 * bit)

    barrier = pltpu.get_barrier_semaphore()
    pl.semaphore_signal(barrier, inc=1, device_id=(partner,), device_id_type=MESH_ID)
    for axis in range(3):
        weight = axis_weight(axis)
        peer = me + weight * (1 - 2 * ((me // weight) % 2))
        pl.semaphore_signal(barrier, inc=1, device_id=(peer,), device_id_type=MESH_ID)

    def columns(half, chunk):
        return pl.ds(pl.multiple_of((half * PER_MAT + chunk % PER_MAT) * CW, CW), CW)

    def start_slab(half, chunk, buf):
        @pl.when(chunk < PER_MAT)
        def _():
            pltpu.make_async_copy(h_hbm.at[:, columns(half, chunk)], slab.at[buf], slab_sem.at[buf]).start()

        @pl.when(chunk >= PER_MAT)
        def _():
            pltpu.make_async_copy(a_hbm.at[:, columns(half, chunk)], slab.at[buf], slab_sem.at[buf]).start()

    def wait_slab(buf):
        pltpu.make_async_copy(h_hbm.at[:, pl.ds(0, CW)], slab.at[buf], slab_sem.at[buf]).wait()

    n_pieces = gt_hbm.shape[0] // CW

    def x_copy(q):
        rows = pl.ds(q * 512, 512)
        return pltpu.make_async_copy(xt_hbm.at[rows, :], lt.at[0, rows, :], g_sem.at[1 + q])

    def g_copy(piece):
        return pltpu.make_async_copy(gt_hbm.at[pl.ds(pl.multiple_of(piece * CW, CW), CW), :], gpiece, g_sem.at[0])

    start_slab(1 - core, 0, 0)
    for q in range(4):
        x_copy(q).start()
    start_slab(core, 0, 2)

    def load_clip(chunk, buf):
        scale = jnp.where(chunk < PER_MAT, rowf[...], 1.0)
        clip[...] = (slab[buf].astype(F32) * scale).astype(BF16)

    def partner_chunk(chunk, opening=False):
        buf = chunk % 2
        wait_slab(buf)
        load_clip(chunk, buf)

        @pl.when(chunk + 1 < CHUNKS)
        def _():
            start_slab(1 - core, chunk + 1, 1 - buf)

        mat = chunk // PER_MAT
        for q in range(4):
            rows = pl.ds(q * 512, 512)
            if opening:
                x_copy(q).wait()
            s0s[buf, rows, :] = jnp.dot(lt[mat, rows, :], clip[...], preferred_element_type=F32).astype(BF16)

    def d2d(chunk):
        buf = chunk % 2
        return pltpu.make_async_remote_copy(s0s.at[buf], s0r.at[buf], d_send.at[buf], d_recv.at[buf], device_id=(partner,), device_id_type=MESH_ID)

    def own_chunk(chunk):
        buf = 2 + chunk % 2
        wait_slab(buf)
        load_clip(chunk, buf)

        @pl.when(chunk + 1 < CHUNKS)
        def _():
            start_slab(core, chunk + 1, 5 - buf)

        d2d(chunk).wait()
        mat = chunk // PER_MAT
        for q in range(4):
            rows = pl.ds(q * 512, 512)
            part = jnp.dot(lt[mat, rows, :], clip[...], preferred_element_type=F32)
            own[chunk % OWN, rows, :] = (part + s0r[chunk % 2, rows, :].astype(F32)).astype(BF16)

    def kept_row(chunk, stage):
        row = 0
        for s in range(stage):
            bit, _ = bit_peer(chunk, s)
            row = row + bit * (1024 // (2 ** s))
        return row

    recv_bufs = (rc1, rc2, rc3)

    def stage_copy(chunk, stage):
        size = 1024 // (2 ** stage)
        bit, peer = bit_peer(chunk, stage)
        row = kept_row(chunk, stage) + (1 - bit) * size
        slot = chunk % RECV
        return pltpu.make_async_remote_copy(
            own.at[chunk % OWN, pl.ds(pl.multiple_of(row, CW), size), :], recv_bufs[stage].at[slot],
            sems_s.at[stage, slot], sems_r.at[stage, slot], device_id=(peer,), device_id_type=MESH_ID)

    def stage_sum(chunk, stage):
        size = 1024 // (2 ** stage)
        rows = pl.ds(pl.multiple_of(kept_row(chunk, stage + 1), CW), size)
        return rows, own[chunk % OWN, rows, :].astype(F32) + recv_bufs[stage][chunk % RECV].astype(F32)

    def start_out(chunk):
        low = 0
        for out, high in zip(outs, bounds):
            @pl.when((chunk >= low) & (chunk < high))
            def _():
                pltpu.make_async_copy(obuf.at[chunk % 2], out.at[chunk - low], o_sem.at[chunk % 2]).start()

            low = high

    def wait_out(chunk):
        pltpu.make_async_copy(obuf.at[chunk % 2], outs[0].at[0], o_sem.at[chunk % 2]).wait()

    partner_chunk(0, True)
    g_copy(0).start()
    pl.semaphore_wait(barrier, 4)
    d2d(0).start()

    def step(t, _):
        @pl.when(t >= LAG3)
        def _():
            chunk = t - LAG3
            stage_copy(chunk, 2).wait()
            _, total = stage_sum(chunk, 2)

            @pl.when(chunk >= 2)
            def _():
                wait_out(chunk - 2)

            @pl.when(chunk < PER_MAT)
            def _():
                obuf[chunk % 2] = total.astype(BF16)

            @pl.when(chunk >= PER_MAT)
            def _():
                obuf[chunk % 2] = total.T.astype(BF16)

            start_out(chunk)

        @pl.when((t >= LAG2) & (t < CHUNKS + LAG2))
        def _():
            chunk = t - LAG2
            stage_copy(chunk, 1).wait()
            rows, total = stage_sum(chunk, 1)
            own[chunk % OWN, rows, :] = total.astype(BF16)

        @pl.when((t >= LAG1) & (t < CHUNKS + LAG1))
        def _():
            chunk = t - LAG1
            stage_copy(chunk, 0).wait()
            rows, total = stage_sum(chunk, 0)
            own[chunk % OWN, rows, :] = total.astype(BF16)

        @pl.when((t >= 1) & (t < CHUNKS + 1))
        def _():
            stage_copy(t - 1, 0).start()

        @pl.when(t < n_pieces)
        def _():
            g_copy(t).wait()
            lt[1, pl.ds(pl.multiple_of(t * CW, CW), CW), :] = (gpiece[...].astype(F32) * colf[...]).astype(BF16)

            @pl.when(t + 1 < n_pieces)
            def _():
                g_copy(t + 1).start()

        @pl.when(t < CHUNKS - 1)
        def _():
            partner_chunk(t + 1)

        @pl.when(t < CHUNKS)
        def _():
            own_chunk(t)

        @pl.when(t < CHUNKS - 1)
        def _():
            d2d(t + 1).start()

        @pl.when((t >= LAG1) & (t < CHUNKS + LAG1))
        def _():
            stage_copy(t - LAG1, 1).start()

        @pl.when((t >= LAG2) & (t < CHUNKS + LAG2))
        def _():
            stage_copy(t - LAG2, 2).start()

        return 0

    lax.fori_loop(0, CHUNKS + LAG3, step, 0)
    wait_out(CHUNKS - 2)
    wait_out(CHUNKS - 1)


def block_sums(layer, bounds, x_turned, h_rows, a_rows, g_turned, factors):
    dim, n_rows = x_turned.shape
    scratch = [
        pltpu.VMEM((2, dim, n_rows), BF16), pltpu.VMEM((4, n_rows, CW), BF16), pltpu.VMEM((CW, n_rows), BF16), pltpu.VMEM((n_rows, CW), BF16),
        pltpu.VMEM((OWN, dim, CW), BF16), pltpu.VMEM((2, dim, CW), BF16), pltpu.VMEM((2, dim, CW), BF16),
        pltpu.VMEM((RECV, dim // 2, CW), BF16), pltpu.VMEM((RECV, dim // 4, CW), BF16), pltpu.VMEM((RECV, dim // 8, CW), BF16),
        pltpu.VMEM((2, CW, CW), BF16),
        pltpu.SemaphoreType.DMA((4,)), pltpu.SemaphoreType.DMA((5,)), pltpu.SemaphoreType.DMA((2,)),
        pltpu.SemaphoreType.DMA((2,)), pltpu.SemaphoreType.DMA((2,)), pltpu.SemaphoreType.DMA((3, RECV)), pltpu.SemaphoreType.DMA((3, RECV)),
    ]
    flops = 4 * n_rows * dim * h_rows.shape[1]
    sizes = [high - low for low, high in zip((0,) + bounds, bounds)]
    return pl.pallas_call(
        functools.partial(sums_kernel, 2 * layer, bounds),
        out_shape=tuple(jax.ShapeDtypeStruct((n, CW, CW), BF16) for n in sizes),
        in_specs=[ANY, ANY, ANY, ANY] + [pl.BlockSpec(memory_space=pltpu.VMEM)] * 2,
        out_specs=(ANY,) * len(sizes),
        scratch_shapes=scratch,
        compiler_params=pltpu.CompilerParams(collective_id=layer, has_side_effects=True, vmem_limit_bytes=60 * 1024 * 1024),
        cost_estimate=pl.CostEstimate(flops=flops, bytes_accessed=4 * n_rows * h_rows.shape[1], transcendentals=0),
        name=f'sums_{layer}',
    )(x_turned, h_rows, a_rows, g_turned, *factors)


def deliver_kernel(shift, piece_ref, out_hbm, copy_sem, s_sem, r_sem):
    me = lax.axis_index('data')
    core = me % 2
    partner = me + 1 - 2 * core
    barrier = pltpu.get_barrier_semaphore()
    pl.semaphore_signal(barrier, inc=1, device_id=(partner,), device_id_type=MESH_ID)
    for axis in range(3):
        weight = axis_weight(axis)
        peer = me + weight * (1 - 2 * ((me // weight) % 2))
        pl.semaphore_signal(barrier, inc=1, device_id=(peer,), device_id_type=MESH_ID)

    def bit_peer(chunk, stage):
        weight = axis_weight((chunk + shift + stage) % 3)
        bit = (me // weight) % 2
        return bit, me + weight * (1 - 2 * bit)

    def block(chunk, stage):
        row = sum(bit_peer(chunk, s)[0] * (1024 // 2 ** s) for s in range(3 - stage))
        return out_hbm.at[chunk, core, pl.ds(pl.multiple_of(row, CW), CW * 2 ** stage), :]

    def other_half(chunk):
        return out_hbm.at[chunk, core, pl.ds(pl.multiple_of((1 - bit_peer(chunk, 0)[0]) * 1024, CW), 1024), :]

    def placed(chunk):
        return pltpu.make_async_copy(piece_ref.at[chunk], block(chunk, 0), copy_sem.at[chunk])

    def remote(chunk, stage):
        if stage == 0:
            source, target, peer = piece_ref.at[chunk], block(chunk, 0), bit_peer(chunk, 2)[1]
        elif stage < 3:
            source, target, peer = block(chunk, stage), block(chunk, stage), bit_peer(chunk, 2 - stage)[1]
        else:
            part = block(chunk, 2) if stage == 3 else other_half(chunk)
            source, target, peer = part, part, partner
        return pltpu.make_async_remote_copy(source, target, s_sem.at[chunk, stage], r_sem.at[chunk, stage], device_id=(peer,), device_id_type=MESH_ID)

    chunks = range(piece_ref.shape[0])
    for chunk in chunks:
        placed(chunk).start()
    pl.semaphore_wait(barrier, 4)
    for chunk in chunks:
        remote(chunk, 0).start()
    for chunk in chunks:
        placed(chunk).wait()
        remote(chunk, 0).wait()
        remote(chunk, 1).start()
    for chunk in chunks:
        remote(chunk, 1).wait()
        remote(chunk, 2).start()
        remote(chunk, 3).start()
    for chunk in chunks:
        remote(chunk, 2).wait()
        remote(chunk, 4).start()
    for chunk in chunks:
        remote(chunk, 3).wait()
        remote(chunk, 4).wait()


def deliver(layer, pieces):
    n = pieces.shape[0]
    return pl.pallas_call(
        functools.partial(deliver_kernel, 2 * layer), out_shape=jax.ShapeDtypeStruct((n, 2, 8 * CW, CW), BF16),
        in_specs=[pl.BlockSpec(memory_space=pltpu.VMEM)], out_specs=ANY, name='deliver',
        scratch_shapes=[pltpu.SemaphoreType.DMA((n,)), pltpu.SemaphoreType.DMA((n, 5)), pltpu.SemaphoreType.DMA((n, 5))],
        compiler_params=pltpu.CompilerParams(collective_id=2, has_side_effects=True),
        cost_estimate=pl.CostEstimate(flops=40_000_000_000, bytes_accessed=n * 32 * CW * CW, transcendentals=0))(pieces)


def owner_of(chunk, piece, half, shift):
    color = (chunk + shift) % 3
    b1, b2, b3 = piece // 4, (piece // 2) % 2, piece % 2
    return b1 * axis_weight(color) + b2 * axis_weight((color + 1) % 3) + b3 * axis_weight((color + 2) % 3) + half


def finish_kernel(n_in, scale, *refs):
    pieces, noise, out = refs[:n_in], refs[n_in], refs[-1]
    across = out.shape[2] // CW
    for i in range(n_in):
        rows, cols = pl.ds(i // across * CW, CW), pl.ds(i % across * CW, CW)
        out[0, rows, cols] = (pieces[i][0, 0].astype(F32) + noise[0, rows, cols]) * scale


def finish_call(name, layer, grid, piece_specs, tile, gathered, noise, prev, batch_total):
    in_specs = piece_specs + [tile]
    args = [gathered] * len(piece_specs) + [noise]
    aliases = {}
    if prev is not None:
        in_specs.append(ANY)
        args.append(prev)
        aliases = {len(args) - 1: 0}
    steps = grid[0] * grid[1]
    size = steps * tile.block_shape[1] * tile.block_shape[2]
    return pl.pallas_call(
        functools.partial(finish_kernel, len(piece_specs), 1.0 / batch_total),
        out_shape=jax.ShapeDtypeStruct(noise.shape, F32), grid=grid, in_specs=in_specs, out_specs=tile,
        input_output_aliases=aliases, name=f'{name}_{layer}',
        cost_estimate=pl.CostEstimate(flops=size * 200, bytes_accessed=size * 10, transcendentals=0),
        compiler_params=pltpu.CompilerParams(vmem_limit_bytes=50 * 1024 * 1024))(*args)


def finish_up(layer, gathered, offset, start, n, noise, prev, batch_total):
    layers, dim, ff = noise.shape
    shift, across = 2 * layer, 2

    def piece_spec(piece, c):
        def index(k, group):
            chunk = start + across * group + c
            if offset is None:
                return chunk, k, piece, 0
            return owner_of(chunk, piece, k, shift), chunk - offset, 0, 0

        return pl.BlockSpec((1, 1, CW, CW), index)

    tile = pl.BlockSpec((1, dim, across * CW), lambda k, group: (layer, 0, (k * PER_MAT + start) // across + group))
    specs = [piece_spec(piece, c) for piece in range(dim // CW) for c in range(across)]
    return finish_call('finish_up', layer, (2, n // across), specs, tile, gathered, noise, prev, batch_total)


def finish_down(layer, gathered, offset, start, n, noise, prev, batch_total):
    layers, ff, dim = noise.shape
    shift, n_in = 2 * layer, dim // CW

    def piece_spec(d, i):
        def index(k, c):
            chunk = start + 2 * c + d
            return owner_of(chunk, i, k, shift), chunk - offset, 0, 0

        return pl.BlockSpec((1, 1, CW, CW), index)

    tile = pl.BlockSpec((1, 2 * CW, dim), lambda k, c: (layer, (k * PER_MAT + start - PER_MAT) // 2 + c, 0))
    specs = [piece_spec(d, i) for d in range(2) for i in range(n_in)]
    return finish_call('finish_down', layer, (2, n // 2), specs, tile, gathered, noise, prev, batch_total)


def per_device(x_in, dy_out, lengths, w_up, w_down, noise_up, noise_down, clip_norm, batch_total):
    n_samples, seq_len, dim = x_in.shape
    n_rows = n_samples * seq_len
    x_first = x_in.reshape(n_rows, dim)
    z_first, a_first, a_last, h_last, row_f, col_f, x_turned, g_turned, g_last = first_pass(x_first, dy_out.reshape(n_rows, dim), w_up, w_down, clip_norm, lengths)
    piece, = block_sums(1, (CHUNKS,), x_turned, h_last, a_last, g_turned, (row_f, col_f))
    gathered_last = lax.all_gather(piece, 'data')
    g_first = add_product(1, g_last, h_last, w_up, True)
    h_first, row_f, col_f, x_turned, g_turned = block_grad(x_first, g_first, z_first, a_first, w_down, clip_norm, n_samples)
    early, piece_a, piece_b = block_sums(0, BOUNDS, x_turned, h_first, a_first, g_turned, (row_f, col_f))
    first, second, _ = BOUNDS
    part_a, part_b = [lax.all_gather(part, 'data') for part in (piece_a, piece_b)]
    early = deliver(0, early)
    gathered_last, early = lax.optimization_barrier((gathered_last, early))
    grad_up = finish_up(1, gathered_last, 0, 0, PER_MAT, noise_up, None, batch_total)
    grad_down = finish_down(1, gathered_last, 0, PER_MAT, PER_MAT, noise_down, None, batch_total)
    grad_up = finish_up(0, early, None, 0, first, noise_up, grad_up, batch_total)
    grad_up, grad_down, part_a = lax.optimization_barrier((grad_up, grad_down, part_a))
    grad_up = finish_up(0, part_a, first, first, PER_MAT - first, noise_up, grad_up, batch_total)
    grad_down = finish_down(0, part_a, first, PER_MAT, second - PER_MAT, noise_down, grad_down, batch_total)
    grad_up, grad_down, part_b = lax.optimization_barrier((grad_up, grad_down, part_b))
    grad_down = finish_down(0, part_b, second, second, CHUNKS - second, noise_down, grad_down, batch_total)
    return grad_up, grad_down


def solution(mesh):
    batch_spec = P('data', None, None)

    def grad_step(x_in, dy_out, lengths, w_up, w_down, noise_up, noise_down, clip_norm):
        device_fn = functools.partial(per_device, batch_total=x_in.shape[0])
        mapped = jax.shard_map(device_fn, mesh=mesh, in_specs=(batch_spec, batch_spec, P('data'), P(), P(), P(), P(), P()), out_specs=(P(), P()), check_vma=False)
        return mapped(x_in, dy_out, lengths, w_up, w_down, noise_up, noise_down, clip_norm)

    return grad_step
```
